32 devices in a mesh: rep: 2 (over x), gx: 16 (over z, y, core).
Axes of the slice: x: 2, y: 2, z: 4, core: 2. Of those that a mesh axis runs over, the one named last changes fastest.
Arguments:
- positions: float32 [3, 131072], P(None, ('rep', 'gx')), parts along dimension 1, may hold values from 0 to 128, as said below
- polar: float32 [131072], P(('rep', 'gx')), parts along dimension 0, may hold values from 0.25 to 1
- field_ext: float32 [3, 131072], P(None, ('rep', 'gx')), parts along dimension 1, may hold values from -10 to 10
- tile_atom: int32 [131072], P(('rep', 'gx')), parts along dimension 0, may hold values from 0 to 4095, as said below
- tile_list: int32 [1024, 3], P(('rep', 'gx')), parts along dimension 0, may hold values from 0 to 63, as said below
- image_shift: int32 [2, 1024, 3], P(None, ('rep', 'gx')), parts along dimension 1, may hold values from 0 to 1, as said below
Outputs:
- dipoles: float32 [3, 131072], P(None, ('rep', 'gx')), parts along dimension 1
- residual: float32 [3, 131072], P(None, ('rep', 'gx')), parts along dimension 1
The draws below stay inside these ranges and needn't reach their ends.
There are 2 independent parts, one for each index of `rep`. The reference program is written for one: setup_inputs(seed, part) draws one part's arguments, and reference() takes and returns one part's arrays. A program takes and returns all parts, laid end to end along the dimension named above; each array names one. Nothing has to cross between parts.
Inputs may be any that keep to these rules, and one draw needn't show every extreme that they name: `positions`: coordinates lie in a box of 64 by 128 by 64; the atoms of slab s have first coordinate between 4 s and 4 s + 4; no two atoms, and no atom and a periodic image of another, are closer than 1.4. `tile_atom`: for each slab, a permutation of 0 to 4095. `tile_list`: entry 0 of a tile is the tile's own index within its slab. Entry n of a tile of slab s names tile n of slab s if n < 32, else tile n - 32 of slab s + 1 (slab 0 after the last). `image_shift`: offsets along the second and third coordinates in box lengths, one pair for each entry of tile_list; zero for entry 0.
All inputs are finite; a program needn't handle non-finite values.
Results may differ from the reference program's by a relative error of at most 0.0003.
Values sent between devices are 32-bit elements; how exact they have to be, the bound alone decides.
A program may use at most 64 MiB of HBM per device.

```python
import math
import jax
import jax.numpy as jnp
from jax import lax

TILE = 128
TILES_DEV = 32
NB = 3
ITERS = 4
TILES = 512
ATOMS_DEV = 4096
ATOMS = 65536


def atom_order(key):
    slab_count = ATOMS // ATOMS_DEV
    keys = jax.random.split(jax.random.fold_in(key, 11), slab_count)

    def one_slab(slab_key):
        return jax.random.permutation(slab_key, ATOMS_DEV).astype(jnp.int32)
    return jax.vmap(one_slab)(keys).reshape(ATOMS)


def lattice_places():
    slot_ids = jnp.arange(ATOMS, dtype=jnp.int32)
    slab_ids = slot_ids // ATOMS_DEV
    local_ids = slot_ids % ATOMS_DEV
    tile_ids = local_ids // TILE
    within = local_ids % TILE
    rows_z = TILES_DEV // 8
    cell_y = tile_ids // rows_z
    cell_z = tile_ids % rows_z
    layer_id = within // 64
    along_y = within // 8 % 8
    along_z = within % 8
    coord_x = 4 * slab_ids + 2 * layer_id + 1
    coord_y = 2 * (8 * cell_y + along_y) + 1
    coord_z = 2 * (8 * cell_z + along_z) + 1
    return (jnp.stack([coord_x, coord_y, coord_z]).astype(jnp.float32), slab_ids)


def draw_tile_atom(key, part):
    return atom_order(key)


def draw_positions(key, part):
    order_ids = atom_order(key)
    base, slab_ids = lattice_places()
    jitter_key = jax.random.fold_in(key, 23)
    jitter = jax.random.uniform(jitter_key, (3, ATOMS), jnp.float32, -0.3, 0.3)
    placed = base + jitter
    target = slab_ids * ATOMS_DEV + order_ids
    return jnp.zeros((3, ATOMS), jnp.float32).at[:, target].set(placed)


def draw_field_ext(key, part):
    slab_count = ATOMS // ATOMS_DEV
    slab_ids = jnp.arange(ATOMS, dtype=jnp.int32) // ATOMS_DEV
    ramp = slab_ids.astype(jnp.float32) / (slab_count - 1)
    noise = jnp.clip(jax.random.normal(key, (3, ATOMS), jnp.float32), -5.0, 5.0)
    return noise * (0.6 + 1.2 * ramp)


def neighbour_entries(key):
    score_key = jax.random.fold_in(key, 37)
    scores = jax.random.randint(score_key, (TILES, 7), 0, 1 << 20) * 8 + jnp.arange(7, dtype=jnp.int32)[None, :]
    picked = jnp.argsort(scores, axis=1)[:, :NB - 1].astype(jnp.int32) + 1
    step_x = picked // 4
    step_y = picked // 2 % 2
    step_z = picked % 2
    rows_z = TILES_DEV // 8
    tile_ids = jnp.arange(TILES, dtype=jnp.int32) % TILES_DEV
    cell_y = (tile_ids // rows_z)[:, None]
    cell_z = (tile_ids % rows_z)[:, None]
    next_y = cell_y + step_y
    next_z = cell_z + step_z
    image_y = next_y // 8
    image_z = next_z // rows_z
    named = step_x * TILES_DEV + next_y % 8 * rows_z + next_z % rows_z
    lists = jnp.concatenate([tile_ids[:, None], named], axis=1).astype(jnp.int32)
    zeros_col = jnp.zeros((TILES, 1), jnp.int32)
    shifts = jnp.stack([jnp.concatenate([zeros_col, image_y], axis=1), jnp.concatenate([zeros_col, image_z], axis=1)]).astype(jnp.int32)
    return (lists, shifts)


def draw_tile_list(key, part):
    lists, shifts = neighbour_entries(key)
    return lists


def draw_image_shift(key, part):
    lists, shifts = neighbour_entries(key)
    return shifts


def shard_levels(own_key, shape, cuts, least, largest):
    factor_of = 1.0
    for position, blocks in cuts:
        steps = jax.random.uniform(jax.random.fold_in(jax.random.fold_in(own_key, 6), position), (blocks,), jnp.float32, least / len(cuts), largest / len(cuts))
        factor_of = factor_of * jnp.repeat(jnp.exp(steps), shape[position] // blocks).reshape((-1,) + (1,) * (len(shape) - 1 - position))
    return factor_of


def setup_inputs(seed: int = 0, part: int = 0) -> dict:
    splits = jax.random.split(jax.random.key(seed), 7)
    part_splits = jax.random.split(jax.random.fold_in(splits[6], part), 7)
    positions = draw_positions(jax.random.fold_in(jax.random.fold_in(splits[6], part), 71), part)
    polar = jnp.clip(jnp.exp(math.log(1.0) - 1.3862944 * jax.random.uniform(part_splits[1], (ATOMS,), jnp.float32) ** shard_levels(part_splits[1], (ATOMS,), ((0, 16),), -0.2, 0.2)), 0.25, 1.0)
    field_ext = draw_field_ext(jax.random.fold_in(jax.random.fold_in(splits[6], part), 71), part)
    tile_atom = draw_tile_atom(jax.random.fold_in(jax.random.fold_in(splits[6], part), 71), part)
    tile_list = draw_tile_list(jax.random.fold_in(jax.random.fold_in(splits[6], part), 71), part)
    image_shift = draw_image_shift(jax.random.fold_in(jax.random.fold_in(splits[6], part), 71), part)
    return {"positions": positions, "polar": polar, "field_ext": field_ext, "tile_atom": tile_atom, "tile_list": tile_list, "image_shift": image_shift}


thole_factor = 0.39

def pair_block(place_left, root_left, moment_left, place_right, root_right, moment_right, weights, self_flags):
    offset_x = place_right[:, 0, None, :] - place_left[:, 0, :, None]
    offset_y = place_right[:, 1, None, :] - place_left[:, 1, :, None]
    offset_z = place_right[:, 2, None, :] - place_left[:, 2, :, None]
    dist_sq = offset_x * offset_x + offset_y * offset_y + offset_z * offset_z
    tile_width = place_left.shape[2]
    row_ids = lax.broadcasted_iota(jnp.int32, (tile_width, tile_width), 0)
    column_ids = lax.broadcasted_iota(jnp.int32, (tile_width, tile_width), 1)
    same_atom = jnp.logical_and(self_flags[:, None, None] > 0, (row_ids == column_ids)[None])
    dist_sq = jnp.where(same_atom, 1.0, dist_sq)
    inv_dist = lax.rsqrt(dist_sq)
    distance = dist_sq * inv_dist
    damp_arg = thole_factor * dist_sq * distance / (root_left[:, :, None] * root_right[:, None, :])
    decay = jnp.exp(-damp_arg)
    inv_cube = jnp.where(same_atom, 0.0, weights[:, None, None] * inv_dist * inv_dist * inv_dist)
    coeff_three = (1.0 - decay) * inv_cube
    coeff_five = 3.0 * (1.0 - (1.0 + damp_arg) * decay) * inv_cube * inv_dist * inv_dist
    offsets = (offset_x, offset_y, offset_z)
    proj_right = offset_x * moment_right[:, 0, None, :] + offset_y * moment_right[:, 1, None, :] + offset_z * moment_right[:, 2, None, :]
    proj_left = offset_x * moment_left[:, 0, :, None] + offset_y * moment_left[:, 1, :, None] + offset_z * moment_left[:, 2, :, None]
    lift_right = coeff_five * proj_right
    lift_left = coeff_five * proj_left
    field_left = jnp.stack([lax.optimization_barrier(jnp.sum(lift_right * offsets[component] - coeff_three * moment_right[:, component, None, :], axis=2)) for component in range(3)], axis=1)
    field_right = jnp.stack([lax.optimization_barrier(jnp.sum(lift_left * offsets[component] - coeff_three * moment_left[:, component, :, None], axis=1)) for component in range(3)], axis=1)
    return (field_left, field_right)

def slab_fields(window_place, window_root, window_moment, left_index, right_index, image_vec, weights, self_flags):
    entries = left_index.shape[0]
    block_size = math.gcd(entries, 32)
    window_size = window_place.shape[0]
    tile_width = window_place.shape[2]
    slot_ids = jnp.arange(window_size, dtype=jnp.int32)

    def accumulate(summed, first_entry):
        left_rows = lax.dynamic_slice_in_dim(left_index, first_entry, block_size)
        right_rows = lax.dynamic_slice_in_dim(right_index, first_entry, block_size)
        image_rows = lax.dynamic_slice_in_dim(image_vec, first_entry, block_size)
        weight_rows = lax.dynamic_slice_in_dim(weights, first_entry, block_size)
        flag_rows = lax.dynamic_slice_in_dim(self_flags, first_entry, block_size)
        place_left = jnp.take(window_place, left_rows, axis=0)
        place_right = jnp.take(window_place, right_rows, axis=0) + image_rows[:, :, None]
        field_left, field_right = pair_block(place_left, jnp.take(window_root, left_rows, axis=0), jnp.take(window_moment, left_rows, axis=0), place_right, jnp.take(window_root, right_rows, axis=0), jnp.take(window_moment, right_rows, axis=0), weight_rows, flag_rows)
        hit_left = (left_rows[:, None] == slot_ids[None, :]).astype(jnp.float32)
        hit_right = (right_rows[:, None] == slot_ids[None, :]).astype(jnp.float32)
        summed = summed + jnp.einsum('ew,ef->wf', hit_left, field_left.reshape(block_size, 3 * tile_width), precision=lax.Precision.HIGHEST)
        summed = summed + jnp.einsum('ew,ef->wf', hit_right, field_right.reshape(block_size, 3 * tile_width), precision=lax.Precision.HIGHEST)
        return (summed, None)
    first_entries = jnp.arange(0, entries, block_size, dtype=jnp.int32)
    summed, _ = lax.scan(accumulate, jnp.zeros((window_size, 3 * tile_width), jnp.float32), first_entries)
    return summed.reshape(window_size, 3, tile_width)

def image_vectors(lists, shifts, last_flag, tile_count, box_x, box_y, box_z):
    crossing = lists >= tile_count
    wrapped = jnp.where(jnp.logical_and(crossing, last_flag), box_x, 0.0)
    vectors = jnp.stack([wrapped, shifts[0].astype(jnp.float32) * box_y, shifts[1].astype(jnp.float32) * box_z], axis=-1)
    return vectors.reshape(-1, 3)

def reference(positions, polar, field_ext, tile_atom, tile_list, image_shift):
    slab_count = TILES // TILES_DEV
    slot_atom = jnp.arange(ATOMS, dtype=jnp.int32) // ATOMS_DEV * ATOMS_DEV + tile_atom
    tiled_place = positions[:, slot_atom].reshape(3, TILES, TILE).transpose(1, 0, 2)
    tiled_polar = polar[slot_atom].reshape(TILES, TILE)
    tiled_root = jnp.sqrt(tiled_polar)
    tiled_rhs = field_ext[:, slot_atom].reshape(3, TILES, TILE).transpose(1, 0, 2)
    box_x = 4.0 * slab_count
    box_y = 128.0
    box_z = 2.0 * TILES_DEV
    last_flag = (jnp.arange(TILES, dtype=jnp.int32) // TILES_DEV == slab_count - 1)[:, None]
    image_all = image_vectors(tile_list, image_shift, last_flag, TILES_DEV, box_x, box_y, box_z)
    entry_ids = jnp.arange(NB, dtype=jnp.int32)
    own_left = jnp.repeat(jnp.arange(TILES_DEV, dtype=jnp.int32), NB)
    own_weights = jnp.tile(jnp.where(entry_ids == 0, 0.5, 1.0), TILES_DEV)
    own_self = jnp.tile((entry_ids == 0).astype(jnp.int32), TILES_DEV)
    slab_ids = jnp.arange(slab_count, dtype=jnp.int32)

    def apply_operator(moment):

        def per_slab(summed, slab):
            first = slab * TILES_DEV
            after = (slab + 1) % slab_count * TILES_DEV
            window_place = jnp.concatenate([lax.dynamic_slice_in_dim(tiled_place, first, TILES_DEV), lax.dynamic_slice_in_dim(tiled_place, after, TILES_DEV)], axis=0)
            window_root = jnp.concatenate([lax.dynamic_slice_in_dim(tiled_root, first, TILES_DEV), lax.dynamic_slice_in_dim(tiled_root, after, TILES_DEV)], axis=0)
            window_moment = jnp.concatenate([lax.dynamic_slice_in_dim(moment, first, TILES_DEV), lax.dynamic_slice_in_dim(moment, after, TILES_DEV)], axis=0)
            lists = lax.dynamic_slice_in_dim(tile_list, first, TILES_DEV).reshape(-1)
            images = lax.dynamic_slice_in_dim(image_all, first * NB, TILES_DEV * NB)
            window = slab_fields(window_place, window_root, window_moment, own_left, lists, images, own_weights, own_self)
            summed = lax.dynamic_update_slice_in_dim(summed, lax.dynamic_slice_in_dim(summed, first, TILES_DEV) + window[:TILES_DEV], first, 0)
            summed = lax.dynamic_update_slice_in_dim(summed, lax.dynamic_slice_in_dim(summed, after, TILES_DEV) + window[TILES_DEV:], after, 0)
            return (summed, None)
        fields, _ = lax.scan(per_slab, jnp.zeros((TILES, 3, TILE), jnp.float32), slab_ids)
        return moment / tiled_polar[:, None, :] - fields
    solution = jnp.zeros_like(tiled_rhs)
    resid = tiled_rhs
    direction = tiled_rhs
    norm_now = jnp.sum(resid * resid)
    for iteration in range(ITERS):
        applied = apply_operator(direction)
        step_size = norm_now / jnp.sum(direction * applied)
        solution = solution + step_size * direction
        resid = resid - step_size * applied
        norm_next = jnp.sum(resid * resid)
        direction = resid + norm_next / norm_now * direction
        norm_now = norm_next
    dipoles = jnp.zeros((3, ATOMS), jnp.float32).at[:, slot_atom].set(solution.transpose(1, 0, 2).reshape(3, ATOMS))
    residual = jnp.zeros((3, ATOMS), jnp.float32).at[:, slot_atom].set(resid.transpose(1, 0, 2).reshape(3, ATOMS))
    return (dipoles, residual)
```

```python
import functools

import jax
import jax.numpy as jnp
from jax import lax
from jax.experimental import pallas as pl
from jax.experimental.pallas import tpu as pltpu
from jax.sharding import PartitionSpec as P

ITERS = 4
MESH = pl.DeviceIdType.MESH
thole_factor = 0.39
LN2 = 0.6931471805599453
AWAY = 1e28
F32 = jnp.float32
BF16 = jnp.bfloat16


def split_two(value):
    high = value.astype(BF16)
    return high, (value - high.astype(F32)).astype(BF16)


def split_three(value):
    high = value.astype(BF16)
    rest = value - high.astype(F32)
    middle = rest.astype(BF16)
    return high, middle, (rest - middle.astype(F32)).astype(BF16)


def gather_tile(row, source, tiles):
    width = 128
    inner = jnp.broadcast_to(row & (width - 1), (8, width))
    outer = jnp.broadcast_to(row >> 7, (8, width))
    value = jnp.zeros((8, width), F32)
    for tile in range(tiles):
        picked = jnp.take_along_axis(
            source[pl.ds(tile * 8, 8), :], inner, axis=1, mode="promise_in_bounds"
        )
        value = jnp.where(outer == tile, picked, value)
    return value


def tiling_kernel(tiles, place_ref, polar_ref, field_ref, atom_ref, out_ref, inverse, feat):
    width = 128
    for tile in range(tiles):
        lanes = pl.ds(tile * width, width)
        feat[tile * 8 : tile * 8 + 3, :] = place_ref[:, lanes]
        feat[tile * 8 + 3 : tile * 8 + 6, :] = field_ref[:, lanes]
        feat[tile * 8 + 6 : tile * 8 + 7, :] = polar_ref[:, lanes]
        feat[tile * 8 + 7 : tile * 8 + 8, :] = jnp.ones((1, width), F32)
    sub_ids = lax.broadcasted_iota(jnp.int32, (8, width), 0)

    def fill(tile, carry):
        value = gather_tile(atom_ref[pl.ds(tile, 1), :], feat, tiles)
        root = lax.rsqrt(value)
        value = jnp.where(sub_ids == 7, pltpu.roll(root, 1, 0), value)
        out_ref[pl.ds(pl.multiple_of(tile * 8, 8), 8), :] = value
        return carry

    lax.fori_loop(0, tiles, fill, 0, unroll=4)

    lane_ids = lax.broadcasted_iota(jnp.int32, (width, width), 0)
    tile_ids = lax.broadcasted_iota(jnp.int32, (tiles, width), 0)
    lane_row = lax.broadcasted_iota(jnp.int32, (tiles, width), 1).astype(F32)

    def invert(tile, total):
        row = atom_ref[pl.ds(tile, 1), :]
        outer = tile_ids == (row >> 7)
        number = jnp.full((tiles, width), tile, jnp.int32).astype(F32)
        left = jnp.concatenate(
            [jnp.where(outer, number, 0.0), jnp.where(outer, lane_row, 0.0)], axis=0
        ).astype(BF16)
        right = jnp.where(lane_ids == (row & (width - 1)), 1.0, 0.0).astype(BF16)
        return total + lax.dot_general(
            left, right, (((1,), (1,)), ((), ())), preferred_element_type=F32
        )

    found = lax.fori_loop(
        0, tiles, invert, jnp.zeros((2 * tiles, width), F32), unroll=4
    )
    inverse[...] = (found[:tiles] * float(width) + found[tiles:]).astype(jnp.int32)


def untiling_kernel(tiles, tiled_ref, inverse, dip_ref, res_ref):
    width = 128

    def give(tile, carry):
        value = gather_tile(inverse[pl.ds(tile, 1), :], tiled_ref, tiles)
        lanes = pl.ds(pl.multiple_of(tile * width, width), width)
        dip_ref[:, lanes] = value[0:3]
        res_ref[:, lanes] = value[3:6]
        return carry

    lax.fori_loop(0, tiles, give, 0, unroll=4)


def eight(index):
    return pl.ds(pl.multiple_of(index * 8, 8), 8)


def kernel(
    count,
    tiles,
    links,
    list_ref,
    shift_ref,
    names_ref,
    tiled_ref,
    out_ref,
    window,
    middle,
    placed,
    centred,
    local,
    away,
    pair_own,
    pair_back,
    pair_left,
    bases,
    coefs,
    vectors,
    blocks,
    fields,
    summed,
    sent_w,
    ahead_w,
    sent_f,
    back_f,
    dots,
    pack_sem,
    w_sem,
    f_sem,
    dot_sem,
):
    width = 128
    near = links - 1
    slots = near * tiles
    me = lax.axis_index("gx")
    after = lax.rem(me + 1, count)
    before = lax.rem(me + count - 1, count)

    barrier = pltpu.get_barrier_semaphore()

    def greet(step, carry):
        pl.semaphore_signal(
            barrier, inc=1, device_id={"gx": lax.rem(me + step, count)}, device_id_type=MESH
        )
        return carry

    lax.fori_loop(1, count, greet, 0)

    sub_ids = lax.broadcasted_iota(jnp.int32, (8, width), 0)
    low_rows = sub_ids < 4

    window[0 : tiles * 8, :] = tiled_ref[...]
    pl.semaphore_wait(barrier, count - 1)
    pack_copy = pltpu.make_async_remote_copy(
        src_ref=tiled_ref,
        dst_ref=window.at[pl.ds(tiles * 8, tiles * 8)],
        send_sem=pack_sem.at[0],
        recv_sem=pack_sem.at[1],
        device_id={"gx": before},
        device_id_type=MESH,
    )
    pack_copy.start()

    row_ids = lax.broadcasted_iota(jnp.int32, (width, width), 0)
    column_ids = lax.broadcasted_iota(jnp.int32, (width, width), 1)
    away[...] = jnp.where(row_ids == column_ids, AWAY, 0.0)

    def strided(first, row):
        return pl.ds(first * 8 + row, tiles, stride=8)

    def centre(first):
        whole = slice(first, first + tiles)
        ones = jnp.ones((tiles, width), F32)
        for axis in range(3):
            here = window[strided(first, axis), :]
            mean = jnp.floor(jnp.mean(here, axis=1, keepdims=True) + 0.5)
            mean = jnp.broadcast_to(mean, here.shape)
            middle[strided(first, axis), :] = mean
            here = here - mean
            local[axis, whole, :] = here
            bases[strided(first, axis), :] = here
            bases[strided(first, axis + 4), :] = here
        bases[strided(first, 3), :] = ones
        bases[strided(first, 7), :] = ones
        for row in range(3, 8):
            middle[strided(first, row), :] = jnp.zeros((tiles, width), F32)
        for tile in range(first, first + tiles):
            placed[tile] = window[tile * 8 : tile * 8 + 8, :]
            centred[tile] = middle[tile * 8 : tile * 8 + 8, :]

    def pair_rows(columns, other, factor, first, same):
        rows = slice(first, first + 16)
        off_x = other[0:1, :] - columns[rows, 0:1]
        off_y = other[1:2, :] - columns[rows, 1:2]
        off_z = other[2:3, :] - columns[rows, 2:3]
        dist_sq = off_x * off_x + off_y * off_y + off_z * off_z
        if same:
            dist_sq = dist_sq + away[rows, :]
        inv = lax.rsqrt(dist_sq)
        inv_sq = inv * inv
        inv_cube = inv_sq * inv
        cube = dist_sq * (dist_sq * inv)
        scale = columns[rows, 7:8] * factor
        decay = jnp.exp(-(scale * cube))
        three = inv_cube - inv_cube * decay
        five = inv_sq * (three - scale * decay)
        return three, five

    def store_pair(target, index, first, three, five):
        rows = slice(first, first + 16)
        more = slice(width + first, width + first + 16)
        high, low = split_two(five)
        target[index, rows, 0:width] = high
        target[index, rows, width : 2 * width] = low
        high, low = split_two(three)
        target[index, more, 0:width] = high
        target[index, more, width : 2 * width] = low

    def put_coefs(index, shift):
        def row(at):
            return jnp.broadcast_to(-shift[at : at + 1, :], (8, width))

        coefs[index, 0] = jnp.where(low_rows, row(0), 1.0)
        coefs[index, 1] = jnp.where(low_rows, row(1), row(2))
        coefs[index, 2] = shift

    def own_pairs(tile):
        here = window[eight(tile), :]
        columns = here.T
        factor = thole_factor * here[7:8, :]
        for first in range(0, width, 16):
            three, five = pair_rows(columns, here, factor, first, True)
            store_pair(pair_own, tile, first, three, five)
        put_coefs(tile, here - middle[eight(tile), :])

    def grouped(size, body):
        def step(group, carry):
            for offset in range(size):
                body(group * size + offset)
            return carry

        lax.fori_loop(0, tiles // size, step, 0)

    centre(0)
    grouped(2, own_pairs)

    pack_copy.wait_recv()
    centre(tiles)

    lengths = (jnp.where(me == count - 1, 4.0 * count, 0.0), 128.0, 2.0 * tiles)

    def far_pairs(tile):
        here = window[eight(tile), :]
        here_middle = middle[eight(tile), :]
        columns = here.T
        for entry in range(near):
            slot = entry * tiles + tile
            named = list_ref[entry + 1, tile]
            crossing = jnp.full((8, width), named, jnp.int32) >= tiles
            moves = jnp.where(
                sub_ids == 0,
                jnp.where(crossing, lengths[0], 0.0),
                jnp.where(
                    sub_ids == 1,
                    shift_ref[entry + 1, 0, tile].astype(F32) * lengths[1],
                    jnp.where(sub_ids == 2, shift_ref[entry + 1, 1, tile].astype(F32) * lengths[2], 0.0),
                ),
            )
            other = placed[named] + moves
            put_coefs(tiles + slot, other - here_middle)
            put_coefs(tiles + slots + slot, here - (centred[named] + moves))
            factor = thole_factor * other[7:8, :]
            for first in range(0, width, 16):
                three, five = pair_rows(columns, other, factor, first, False)
                store_pair(pair_back, slot, first, three, five)
            for part in (slice(0, width), slice(width, 2 * width)):
                for half in (slice(0, width), slice(width, 2 * width)):
                    pair_left[slot, part, half] = pair_back[slot, part, half].T

    grouped(1, far_pairs)

    named_row = jnp.concatenate(
        [names_ref[entry + 1 : entry + 2, :] for entry in range(near)] * 3, axis=1
    )
    window_ids = lax.broadcasted_iota(jnp.int32, (2 * tiles, 3 * slots), 0)
    hits = jnp.where(window_ids == named_row, 1.0, 0.0).astype(BF16)

    alpha_inv = 1.0 / window[strided(0, 6), :]

    def put_vector(first, vec):
        whole = slice(first, first + tiles)
        along = local[0, whole, :] * vec[0] + local[1, whole, :] * vec[1] + local[2, whole, :] * vec[2]
        for axis in range(3):
            vectors[strided(first, axis), :] = 3.0 * vec[axis]
            vectors[strided(first, axis + 4), :] = -vec[axis]
        vectors[strided(first, 3), :] = 3.0 * along

    vectors[...] = jnp.zeros_like(vectors)

    def make_block(tile):
        base = bases[eight(tile), :]
        vec = vectors[eight(tile), :]

        def row(at):
            return jnp.broadcast_to(vec[at : at + 1, :], (8, width))

        moments = jnp.concatenate(
            [
                base * jnp.where(low_rows, row(0), row(3)),
                base * jnp.where(low_rows, row(1), row(2)),
            ],
            axis=0,
        )
        minus = jnp.concatenate([jnp.where(low_rows, 0.0, vec), jnp.zeros((8, width), F32)], axis=0)
        for part, value in enumerate(split_three(moments)):
            blocks[tile, part * 16 : part * 16 + 16, 0:width] = value
        for part, value in enumerate(split_three(minus)):
            blocks[tile, part * 16 : part * 16 + 16, width : 2 * width] = value

    def product(tile, weights, index):
        out = jnp.dot(blocks[tile], weights, preferred_element_type=F32)
        out = out[:, :width] + out[:, width:]
        out = (out[0:16] + out[16:32]) + out[32:48]
        total = coefs[index, 0] * out[0:8] + coefs[index, 1] * out[8:16]
        total = total + pltpu.roll(total, 4, 0)
        return total - coefs[index, 2] * jnp.broadcast_to(total[3:4, :], (8, width))

    def copy_w(turn):
        return pltpu.make_async_remote_copy(
            src_ref=sent_w.at[turn],
            dst_ref=ahead_w.at[turn],
            send_sem=w_sem.at[0, turn],
            recv_sem=w_sem.at[1, turn],
            device_id={"gx": before},
            device_id_type=MESH,
        )

    def copy_f(turn):
        return pltpu.make_async_remote_copy(
            src_ref=sent_f.at[turn],
            dst_ref=back_f.at[turn],
            send_sem=f_sem.at[0, turn],
            recv_sem=f_sem.at[1, turn],
            device_id={"gx": after},
            device_id_type=MESH,
        )

    def back_step(tile):
        make_block(tile)
        for entry in range(near):
            slot = entry * tiles + tile
            fields[eight(slot), :] = product(tile, pair_back[slot], tiles + slot)

    def own_step(tile):
        summed[eight(tile), :] = product(tile, pair_own[tile], tile)

    def left_step(tile):
        total = summed[eight(tile), :]
        for entry in range(near):
            slot = entry * tiles + tile
            named = list_ref[entry + 1, tile]
            total = total + product(named, pair_left[slot], tiles + slots + slot)
        summed[eight(tile), :] = total

    def applied(turn, vec):
        put_vector(0, vec)
        grouped(8, back_step)
        back = jnp.concatenate(
            [fields[pl.ds(axis, slots, stride=8), :] for axis in range(3)], axis=1
        )
        spread = jnp.dot(
            hits, jnp.concatenate(split_three(back), axis=0), preferred_element_type=F32
        )
        for axis in range(3):
            sent_f[turn, axis] = spread[tiles:, axis * width : (axis + 1) * width]
        copy_f(turn).start()
        grouped(16, own_step)
        if turn == 0:
            ahead = [window[strided(tiles, 3 + axis), :] for axis in range(3)]
        else:
            copy_w(turn).wait_recv()
            ahead = [ahead_w[turn, axis] for axis in range(3)]
        put_vector(tiles, ahead)
        for tile in range(tiles):
            make_block(tiles + tile)
        grouped(8, left_step)
        field = [
            summed[strided(0, axis), :] + spread[:tiles, axis * width : (axis + 1) * width]
            for axis in range(3)
        ]
        copy_f(turn).wait_recv()
        return [vec[axis] * alpha_inv - (field[axis] + back_f[turn, axis]) for axis in range(3)]

    def dot_rows(left, right):
        total = left[0] * right[0] + left[1] * right[1] + left[2] * right[2]
        return jnp.sum(total, axis=0, keepdims=True)

    def send_dots(turn, resid, w):
        dots[turn, 0] = jnp.where(
            sub_ids == 0, dot_rows(resid, resid), jnp.where(sub_ids == 1, dot_rows(resid, w), 0.0)
        )

        def send(step, carry):
            pltpu.make_async_remote_copy(
                src_ref=dots.at[turn, 0],
                dst_ref=dots.at[turn, step],
                send_sem=dot_sem.at[0, turn],
                recv_sem=dot_sem.at[1, turn],
                device_id={"gx": lax.rem(me + step, count)},
                device_id_type=MESH,
            ).start()
            return carry

        lax.fori_loop(1, count, send, 0)

    def wait_dots(turn, which):
        whole = dots.at[turn, pl.ds(1, count - 1)]
        pltpu.make_async_copy(whole, whole, dot_sem.at[which, turn]).wait()

    resid = [window[strided(0, 3 + axis), :] for axis in range(3)]
    w = applied(0, resid)
    solution = direction = s = z = None
    norm_last = step_last = None
    for turn in range(ITERS):
        more_turns = turn + 1 < ITERS
        if more_turns:
            for axis in range(3):
                sent_w[turn + 1, axis] = w[axis]
            copy_w(turn + 1).start()
        send_dots(turn, resid, w)
        if more_turns:
            q = applied(turn + 1, w)
        wait_dots(turn, 1)
        sums = jnp.sum(jnp.sum(dots[turn], axis=0), axis=1, keepdims=True)
        norm = sums[0:1, :]
        product_now = sums[1:2, :]
        if turn == 0:
            step = norm / product_now
            direction, s = resid, w
            solution = [step * direction[axis] for axis in range(3)]
            if more_turns:
                z = q
        else:
            ratio = norm / norm_last
            step = norm / (product_now - ratio * norm / step_last)
            direction = [resid[axis] + ratio * direction[axis] for axis in range(3)]
            s = [w[axis] + ratio * s[axis] for axis in range(3)]
            solution = [solution[axis] + step * direction[axis] for axis in range(3)]
            if more_turns:
                z = [q[axis] + ratio * z[axis] for axis in range(3)]
        resid = [resid[axis] - step * s[axis] for axis in range(3)]
        if more_turns:
            w = [w[axis] - step * z[axis] for axis in range(3)]
        norm_last, step_last = norm, step

    for axis in range(3):
        out_ref[strided(0, axis), :] = solution[axis]
        out_ref[strided(0, 3 + axis), :] = resid[axis]
    out_ref[strided(0, 6), :] = jnp.zeros((tiles, width), F32)
    out_ref[strided(0, 7), :] = jnp.zeros((tiles, width), F32)

    pack_copy.wait_send()
    for turn in range(ITERS):
        if turn > 0:
            copy_w(turn).wait_send()
        copy_f(turn).wait_send()
        wait_dots(turn, 0)


def on_device(positions, polar, field_ext, tile_atom, tile_list, image_shift):
    tiles, links = tile_list.shape
    atoms = tile_atom.shape[0]
    width = atoms // tiles
    near = links - 1
    count = lax.axis_size("gx")
    pairs = (2 * width, 2 * width)
    vmem = pl.BlockSpec(memory_space=pltpu.VMEM)
    smem = pl.BlockSpec(memory_space=pltpu.SMEM)
    out = jax.ShapeDtypeStruct((3, atoms), F32)
    vectors = pltpu.VMEM((ITERS, 3, tiles, width), F32)
    tiled = jax.ShapeDtypeStruct((tiles * 8, width), F32)
    per_window = pltpu.VMEM((2 * tiles * 8, width), F32)
    window, inverse = pl.pallas_call(
        functools.partial(tiling_kernel, tiles),
        out_shape=(tiled, jax.ShapeDtypeStruct((tiles, width), jnp.int32)),
        in_specs=[vmem, vmem, vmem, vmem],
        out_specs=(vmem, vmem),
        scratch_shapes=[pltpu.VMEM((tiles * 8, width), F32)],
    )(positions, polar.reshape(1, atoms), field_ext, tile_atom.reshape(tiles, width))
    names = tile_list.T
    found = pl.pallas_call(
        functools.partial(kernel, count, tiles, links),
        out_shape=tiled,
        in_specs=[smem, smem, vmem, vmem],
        out_specs=vmem,
        scratch_shapes=[
            per_window,
            per_window,
            pltpu.VMEM((2 * tiles, 8, width), F32),
            pltpu.VMEM((2 * tiles, 8, width), F32),
            pltpu.VMEM((3, 2 * tiles, width), F32),
            pltpu.VMEM((width, width), F32),
            pltpu.VMEM((tiles,) + pairs, BF16),
            pltpu.VMEM((near * tiles,) + pairs, BF16),
            pltpu.VMEM((near * tiles,) + pairs, BF16),
            per_window,
            pltpu.VMEM(((1 + 2 * near) * tiles, 3, 8, width), F32),
            per_window,
            pltpu.VMEM((2 * tiles, 48, 2 * width), BF16),
            pltpu.VMEM((near * tiles * 8, width), F32),
            pltpu.VMEM((tiles * 8, width), F32),
            vectors,
            vectors,
            vectors,
            vectors,
            pltpu.VMEM((ITERS, count, 8, width), F32),
            pltpu.SemaphoreType.DMA((2,)),
            pltpu.SemaphoreType.DMA((2, ITERS)),
            pltpu.SemaphoreType.DMA((2, ITERS)),
            pltpu.SemaphoreType.DMA((2, ITERS)),
        ],
        compiler_params=pltpu.CompilerParams(collective_id=0, has_side_effects=True),
    )(names, image_shift.transpose(2, 0, 1), names, window)
    return pl.pallas_call(
        functools.partial(untiling_kernel, tiles),
        out_shape=(out, out),
        in_specs=[vmem, vmem],
        out_specs=(vmem, vmem),
    )(found, inverse)


def solution(mesh):
    in_specs = (
        P(None, ("rep", "gx")),
        P(("rep", "gx")),
        P(None, ("rep", "gx")),
        P(("rep", "gx")),
        P(("rep", "gx"), None),
        P(None, ("rep", "gx"), None),
    )
    out_specs = (P(None, ("rep", "gx")), P(None, ("rep", "gx")))
    return jax.shard_map(
        on_device, mesh=mesh, in_specs=in_specs, out_specs=out_specs, check_vma=False
    )
```

```python
import functools

import jax
import jax.numpy as jnp
from jax import lax
from jax.experimental import pallas as pl
from jax.experimental.pallas import tpu as pltpu
from jax.sharding import PartitionSpec as P

ITERS = 4
MESH = pl.DeviceIdType.MESH
thole_factor = 0.39
LN2 = 0.6931471805599453
AWAY = 1e28
F32 = jnp.float32
BF16 = jnp.bfloat16


def split_two(value):
    high = value.astype(BF16)
    return high, (value - high.astype(F32)).astype(BF16)


def split_three(value):
    high = value.astype(BF16)
    rest = value - high.astype(F32)
    middle = rest.astype(BF16)
    return high, middle, (rest - middle.astype(F32)).astype(BF16)


def gather_tile(row, source, tiles):
    width = 128
    inner = jnp.broadcast_to(row & (width - 1), (8, width))
    outer = jnp.broadcast_to(row >> 7, (8, width))
    value = jnp.zeros((8, width), F32)
    for tile in range(tiles):
        picked = jnp.take_along_axis(
            source[pl.ds(tile * 8, 8), :], inner, axis=1, mode="promise_in_bounds"
        )
        value = jnp.where(outer == tile, picked, value)
    return value


def tiling_kernel(tiles, place_ref, polar_ref, field_ref, atom_ref, out_ref, inverse, feat):
    width = 128
    for tile in range(tiles):
        lanes = pl.ds(tile * width, width)
        feat[tile * 8 : tile * 8 + 3, :] = place_ref[:, lanes]
        feat[tile * 8 + 3 : tile * 8 + 6, :] = field_ref[:, lanes]
        feat[tile * 8 + 6 : tile * 8 + 7, :] = polar_ref[:, lanes]
        feat[tile * 8 + 7 : tile * 8 + 8, :] = jnp.ones((1, width), F32)
    sub_ids = lax.broadcasted_iota(jnp.int32, (8, width), 0)

    def fill(tile, carry):
        value = gather_tile(atom_ref[pl.ds(tile, 1), :], feat, tiles)
        root = lax.rsqrt(value)
        value = jnp.where(sub_ids == 7, pltpu.roll(root, 1, 0), value)
        out_ref[pl.ds(pl.multiple_of(tile * 8, 8), 8), :] = value
        return carry

    lax.fori_loop(0, tiles, fill, 0, unroll=4)

    lane_ids = lax.broadcasted_iota(jnp.int32, (width, width), 0)
    tile_ids = lax.broadcasted_iota(jnp.int32, (tiles, width), 0)
    lane_row = lax.broadcasted_iota(jnp.int32, (tiles, width), 1).astype(F32)

    def invert(tile, total):
        row = atom_ref[pl.ds(tile, 1), :]
        outer = tile_ids == (row >> 7)
        number = jnp.full((tiles, width), tile, jnp.int32).astype(F32)
        left = jnp.concatenate(
            [jnp.where(outer, number, 0.0), jnp.where(outer, lane_row, 0.0)], axis=0
        ).astype(BF16)
        right = jnp.where(lane_ids == (row & (width - 1)), 1.0, 0.0).astype(BF16)
        return total + lax.dot_general(
            left, right, (((1,), (1,)), ((), ())), preferred_element_type=F32
        )

    found = lax.fori_loop(
        0, tiles, invert, jnp.zeros((2 * tiles, width), F32), unroll=4
    )
    inverse[...] = (found[:tiles] * float(width) + found[tiles:]).astype(jnp.int32)


def untiling_kernel(tiles, tiled_ref, inverse, dip_ref, res_ref):
    width = 128

    def give(tile, carry):
        value = gather_tile(inverse[pl.ds(tile, 1), :], tiled_ref, tiles)
        lanes = pl.ds(pl.multiple_of(tile * width, width), width)
        dip_ref[:, lanes] = value[0:3]
        res_ref[:, lanes] = value[3:6]
        return carry

    lax.fori_loop(0, tiles, give, 0, unroll=4)


def eight(index):
    return pl.ds(pl.multiple_of(index * 8, 8), 8)


def kernel(
    count,
    tiles,
    links,
    list_ref,
    shift_ref,
    names_ref,
    tiled_ref,
    out_ref,
    window,
    middle,
    placed,
    centred,
    local,
    away,
    pair_own,
    pair_back,
    pair_left,
    bases,
    coefs,
    vectors,
    blocks,
    fields,
    summed,
    sent_w,
    ahead_w,
    sent_f,
    back_f,
    dots,
    pack_sem,
    w_sem,
    f_sem,
    dot_sem,
):
    width = 128
    near = links - 1
    slots = near * tiles
    me = lax.axis_index("gx")
    after = lax.rem(me + 1, count)
    before = lax.rem(me + count - 1, count)

    barrier = pltpu.get_barrier_semaphore()

    def greet(step, carry):
        pl.semaphore_signal(
            barrier, inc=1, device_id={"gx": lax.rem(me + step, count)}, device_id_type=MESH
        )
        return carry

    lax.fori_loop(1, count, greet, 0)

    sub_ids = lax.broadcasted_iota(jnp.int32, (8, width), 0)
    low_rows = sub_ids < 4

    window[0 : tiles * 8, :] = tiled_ref[...]
    pl.semaphore_wait(barrier, count - 1)
    pack_copy = pltpu.make_async_remote_copy(
        src_ref=tiled_ref,
        dst_ref=window.at[pl.ds(tiles * 8, tiles * 8)],
        send_sem=pack_sem.at[0],
        recv_sem=pack_sem.at[1],
        device_id={"gx": before},
        device_id_type=MESH,
    )
    pack_copy.start()

    row_ids = lax.broadcasted_iota(jnp.int32, (width, width), 0)
    column_ids = lax.broadcasted_iota(jnp.int32, (width, width), 1)
    away[...] = jnp.where(row_ids == column_ids, AWAY, 0.0)

    def strided(first, row):
        return pl.ds(first * 8 + row, tiles, stride=8)

    def centre(first):
        whole = slice(first, first + tiles)
        ones = jnp.ones((tiles, width), F32)
        for axis in range(3):
            here = window[strided(first, axis), :]
            mean = jnp.floor(jnp.mean(here, axis=1, keepdims=True) + 0.5)
            mean = jnp.broadcast_to(mean, here.shape)
            middle[strided(first, axis), :] = mean
            here = here - mean
            local[axis, whole, :] = here
            bases[strided(first, axis), :] = here
            bases[strided(first, axis + 4), :] = here
        bases[strided(first, 3), :] = ones
        bases[strided(first, 7), :] = ones
        for row in range(3, 8):
            middle[strided(first, row), :] = jnp.zeros((tiles, width), F32)
        for tile in range(first, first + tiles):
            here = window[tile * 8 : tile * 8 + 8, :]
            root = jnp.broadcast_to(here[7:8, :], (8, width))
            placed[tile] = jnp.where(sub_ids < 3, here, jnp.where(sub_ids < 5, 0.0, root))
            centred[tile] = middle[tile * 8 : tile * 8 + 8, :]

    def split_rows(value):
        high = value.astype(BF16).astype(F32)
        rest = value - high
        middle = rest.astype(BF16).astype(F32)
        return high, middle, rest - middle

    def left_rows(tile):
        ones = jnp.ones((24, width), F32)
        return jnp.concatenate([*split_rows(placed[tile]), ones], axis=0).astype(BF16)

    def right_rows(other):
        high, mid, low = split_rows(jnp.where(sub_ids >= 5, other * -thole_factor, other))
        zero = jnp.zeros((8, width), F32)
        parts = []
        for axis in range(3):
            here = sub_ids == axis
            one = jnp.where(here, -1.0, 0.0)
            parts.append(
                [one, one, one] + [jnp.where(here, value, 0.0) for value in (high, mid, low)]
            )
        third = jnp.where(sub_ids == 7, high, 0.0)
        second = jnp.where(sub_ids == 6, mid, third)
        parts.append([jnp.where(sub_ids == 5, low, second), second, third, zero, zero, zero])
        parts = [jnp.concatenate(part, axis=0) for part in parts]
        return jnp.concatenate(parts, axis=1).astype(BF16)

    def offsets(left, right):
        return lax.dot_general(
            left, right, (((0,), (0,)), ((), ())), preferred_element_type=F32
        )

    def pair_rows(found, first, same):
        rows = slice(first, first + 16)
        off_x, off_y, off_z, scale = [
            found[rows, part * width : (part + 1) * width] for part in range(4)
        ]
        dist_sq = off_x * off_x + off_y * off_y + off_z * off_z
        if same:
            dist_sq = dist_sq + away[rows, :]
        inv = lax.rsqrt(dist_sq)
        inv_sq = inv * inv
        inv_cube = inv_sq * inv
        cube = dist_sq * (dist_sq * inv)
        decay = jnp.exp(scale * cube)
        three = inv_cube - inv_cube * decay
        five = inv_sq * (three + scale * decay)
        return three, five

    def store_pair(target, index, first, three, five):
        rows = slice(first, first + 16)
        more = slice(width + first, width + first + 16)
        high, low = split_two(five)
        target[index, rows, 0:width] = high
        target[index, rows, width : 2 * width] = low
        high, low = split_two(three)
        target[index, more, 0:width] = high
        target[index, more, width : 2 * width] = low

    def put_coefs(index, shift):
        def row(at):
            return jnp.broadcast_to(-shift[at : at + 1, :], (8, width))

        coefs[index, 0] = jnp.where(low_rows, row(0), 1.0)
        coefs[index, 1] = jnp.where(low_rows, row(1), row(2))
        coefs[index, 2] = shift

    def own_pairs(tile):
        here = placed[tile]
        found = offsets(left_rows(tile), right_rows(here))
        for first in range(0, width, 16):
            three, five = pair_rows(found, first, True)
            store_pair(pair_own, tile, first, three, five)
        put_coefs(tile, here - centred[tile])

    def grouped(size, body):
        def step(group, carry):
            for offset in range(size):
                body(group * size + offset)
            return carry

        lax.fori_loop(0, tiles // size, step, 0)

    centre(0)
    grouped(8, own_pairs)

    pack_copy.wait_recv()
    centre(tiles)

    lengths = (jnp.where(me == count - 1, 4.0 * count, 0.0), 128.0, 2.0 * tiles)

    def far_pairs(tile):
        here = placed[tile]
        here_middle = centred[tile]
        left = left_rows(tile)
        for entry in range(near):
            slot = entry * tiles + tile
            named = list_ref[entry + 1, tile]
            crossing = jnp.full((8, width), named, jnp.int32) >= tiles
            moves = jnp.where(
                sub_ids == 0,
                jnp.where(crossing, lengths[0], 0.0),
                jnp.where(
                    sub_ids == 1,
                    shift_ref[entry + 1, 0, tile].astype(F32) * lengths[1],
                    jnp.where(sub_ids == 2, shift_ref[entry + 1, 1, tile].astype(F32) * lengths[2], 0.0),
                ),
            )
            other = placed[named] + moves
            put_coefs(tiles + slot, other - here_middle)
            put_coefs(tiles + slots + slot, here - (centred[named] + moves))
            found = offsets(left, right_rows(other))
            for first in range(0, width, 16):
                three, five = pair_rows(found, first, False)
                store_pair(pair_back, slot, first, three, five)
            for part in (slice(0, width), slice(width, 2 * width)):
                for half in (slice(0, width), slice(width, 2 * width)):
                    pair_left[slot, part, half] = pair_back[slot, part, half].T

    grouped(4, far_pairs)

    named_row = jnp.concatenate(
        [names_ref[entry + 1 : entry + 2, :] for entry in range(near)] * 3, axis=1
    )
    window_ids = lax.broadcasted_iota(jnp.int32, (2 * tiles, 3 * slots), 0)
    hits = jnp.where(window_ids == named_row, 1.0, 0.0).astype(BF16)

    alpha_inv = 1.0 / window[strided(0, 6), :]

    def put_vector(first, vec):
        whole = slice(first, first + tiles)
        along = local[0, whole, :] * vec[0] + local[1, whole, :] * vec[1] + local[2, whole, :] * vec[2]
        for axis in range(3):
            vectors[strided(first, axis), :] = 3.0 * vec[axis]
            vectors[strided(first, axis + 4), :] = -vec[axis]
        vectors[strided(first, 3), :] = 3.0 * along

    vectors[...] = jnp.zeros_like(vectors)

    def make_block(tile):
        base = bases[eight(tile), :]
        vec = vectors[eight(tile), :]

        def row(at):
            return jnp.broadcast_to(vec[at : at + 1, :], (8, width))

        moments = jnp.concatenate(
            [
                base * jnp.where(low_rows, row(0), row(3)),
                base * jnp.where(low_rows, row(1), row(2)),
            ],
            axis=0,
        )
        minus = jnp.concatenate([jnp.where(low_rows, 0.0, vec), jnp.zeros((8, width), F32)], axis=0)
        for part, value in enumerate(split_three(moments)):
            blocks[tile, part * 16 : part * 16 + 16, 0:width] = value
        for part, value in enumerate(split_three(minus)):
            blocks[tile, part * 16 : part * 16 + 16, width : 2 * width] = value

    def product(tile, weights, index):
        out = jnp.dot(blocks[tile], weights, preferred_element_type=F32)
        out = out[:, :width] + out[:, width:]
        out = (out[0:16] + out[16:32]) + out[32:48]
        total = coefs[index, 0] * out[0:8] + coefs[index, 1] * out[8:16]
        total = total + pltpu.roll(total, 4, 0)
        return total - coefs[index, 2] * jnp.broadcast_to(total[3:4, :], (8, width))

    def copy_w(turn):
        return pltpu.make_async_remote_copy(
            src_ref=sent_w.at[turn],
            dst_ref=ahead_w.at[turn],
            send_sem=w_sem.at[0, turn],
            recv_sem=w_sem.at[1, turn],
            device_id={"gx": before},
            device_id_type=MESH,
        )

    def copy_f(turn):
        return pltpu.make_async_remote_copy(
            src_ref=sent_f.at[turn],
            dst_ref=back_f.at[turn],
            send_sem=f_sem.at[0, turn],
            recv_sem=f_sem.at[1, turn],
            device_id={"gx": after},
            device_id_type=MESH,
        )

    def back_step(tile):
        make_block(tile)
        for entry in range(near):
            slot = entry * tiles + tile
            fields[eight(slot), :] = product(tile, pair_back[slot], tiles + slot)

    def own_step(tile):
        summed[eight(tile), :] = product(tile, pair_own[tile], tile)

    def left_step(tile):
        total = summed[eight(tile), :]
        for entry in range(near):
            slot = entry * tiles + tile
            named = list_ref[entry + 1, tile]
            total = total + product(named, pair_left[slot], tiles + slots + slot)
        summed[eight(tile), :] = total

    def applied(turn, vec):
        put_vector(0, vec)
        grouped(16, back_step)
        back = jnp.concatenate(
            [fields[pl.ds(axis, slots, stride=8), :] for axis in range(3)], axis=1
        )
        spread = jnp.dot(
            hits, jnp.concatenate(split_three(back), axis=0), preferred_element_type=F32
        )
        for axis in range(3):
            sent_f[turn, axis] = spread[tiles:, axis * width : (axis + 1) * width]
        copy_f(turn).start()
        grouped(32, own_step)
        if turn == 0:
            ahead = [window[strided(tiles, 3 + axis), :] for axis in range(3)]
        else:
            copy_w(turn).wait_recv()
            ahead = [ahead_w[turn, axis] for axis in range(3)]
        put_vector(tiles, ahead)
        for tile in range(tiles):
            make_block(tiles + tile)
        grouped(16, left_step)
        field = [
            summed[strided(0, axis), :] + spread[:tiles, axis * width : (axis + 1) * width]
            for axis in range(3)
        ]
        copy_f(turn).wait_recv()
        return [vec[axis] * alpha_inv - (field[axis] + back_f[turn, axis]) for axis in range(3)]

    def dot_rows(left, right):
        total = left[0] * right[0] + left[1] * right[1] + left[2] * right[2]
        return jnp.sum(total, axis=0, keepdims=True)

    def send_dots(turn, resid, w):
        dots[turn, 0] = jnp.where(
            sub_ids == 0, dot_rows(resid, resid), jnp.where(sub_ids == 1, dot_rows(resid, w), 0.0)
        )

        def send(step, carry):
            pltpu.make_async_remote_copy(
                src_ref=dots.at[turn, 0],
                dst_ref=dots.at[turn, step],
                send_sem=dot_sem.at[0, turn],
                recv_sem=dot_sem.at[1, turn],
                device_id={"gx": lax.rem(me + step, count)},
                device_id_type=MESH,
            ).start()
            return carry

        lax.fori_loop(1, count, send, 0)

    def wait_dots(turn, which):
        whole = dots.at[turn, pl.ds(1, count - 1)]
        pltpu.make_async_copy(whole, whole, dot_sem.at[which, turn]).wait()

    resid = [window[strided(0, 3 + axis), :] for axis in range(3)]
    w = applied(0, resid)
    solution = direction = s = z = None
    norm_last = step_last = None
    for turn in range(ITERS):
        more_turns = turn + 1 < ITERS
        if more_turns:
            for axis in range(3):
                sent_w[turn + 1, axis] = w[axis]
            copy_w(turn + 1).start()
        send_dots(turn, resid, w)
        if more_turns:
            q = applied(turn + 1, w)
        wait_dots(turn, 1)
        sums = jnp.sum(jnp.sum(dots[turn], axis=0), axis=1, keepdims=True)
        norm = sums[0:1, :]
        product_now = sums[1:2, :]
        if turn == 0:
            step = norm / product_now
            direction, s = resid, w
            solution = [step * direction[axis] for axis in range(3)]
            if more_turns:
                z = q
        else:
            ratio = norm / norm_last
            step = norm / (product_now - ratio * norm / step_last)
            direction = [resid[axis] + ratio * direction[axis] for axis in range(3)]
            s = [w[axis] + ratio * s[axis] for axis in range(3)]
            solution = [solution[axis] + step * direction[axis] for axis in range(3)]
            if more_turns:
                z = [q[axis] + ratio * z[axis] for axis in range(3)]
        resid = [resid[axis] - step * s[axis] for axis in range(3)]
        if more_turns:
            w = [w[axis] - step * z[axis] for axis in range(3)]
        norm_last, step_last = norm, step

    for axis in range(3):
        out_ref[strided(0, axis), :] = solution[axis]
        out_ref[strided(0, 3 + axis), :] = resid[axis]
    out_ref[strided(0, 6), :] = jnp.zeros((tiles, width), F32)
    out_ref[strided(0, 7), :] = jnp.zeros((tiles, width), F32)

    pack_copy.wait_send()
    for turn in range(ITERS):
        if turn > 0:
            copy_w(turn).wait_send()
        copy_f(turn).wait_send()
        wait_dots(turn, 0)


def on_device(positions, polar, field_ext, tile_atom, tile_list, image_shift):
    tiles, links = tile_list.shape
    atoms = tile_atom.shape[0]
    width = atoms // tiles
    near = links - 1
    count = lax.axis_size("gx")
    pairs = (2 * width, 2 * width)
    vmem = pl.BlockSpec(memory_space=pltpu.VMEM)
    smem = pl.BlockSpec(memory_space=pltpu.SMEM)
    out = jax.ShapeDtypeStruct((3, atoms), F32)
    vectors = pltpu.VMEM((ITERS, 3, tiles, width), F32)
    tiled = jax.ShapeDtypeStruct((tiles * 8, width), F32)
    per_window = pltpu.VMEM((2 * tiles * 8, width), F32)
    window, inverse = pl.pallas_call(
        functools.partial(tiling_kernel, tiles),
        out_shape=(tiled, jax.ShapeDtypeStruct((tiles, width), jnp.int32)),
        in_specs=[vmem, vmem, vmem, vmem],
        out_specs=(vmem, vmem),
        scratch_shapes=[pltpu.VMEM((tiles * 8, width), F32)],
    )(positions, polar.reshape(1, atoms), field_ext, tile_atom.reshape(tiles, width))
    names = tile_list.T
    found = pl.pallas_call(
        functools.partial(kernel, count, tiles, links),
        out_shape=tiled,
        in_specs=[smem, smem, vmem, vmem],
        out_specs=vmem,
        scratch_shapes=[
            per_window,
            per_window,
            pltpu.VMEM((2 * tiles, 8, width), F32),
            pltpu.VMEM((2 * tiles, 8, width), F32),
            pltpu.VMEM((3, 2 * tiles, width), F32),
            pltpu.VMEM((width, width), F32),
            pltpu.VMEM((tiles,) + pairs, BF16),
            pltpu.VMEM((near * tiles,) + pairs, BF16),
            pltpu.VMEM((near * tiles,) + pairs, BF16),
            per_window,
            pltpu.VMEM(((1 + 2 * near) * tiles, 3, 8, width), F32),
            per_window,
            pltpu.VMEM((2 * tiles, 48, 2 * width), BF16),
            pltpu.VMEM((near * tiles * 8, width), F32),
            pltpu.VMEM((tiles * 8, width), F32),
            vectors,
            vectors,
            vectors,
            vectors,
            pltpu.VMEM((ITERS, count, 8, width), F32),
            pltpu.SemaphoreType.DMA((2,)),
            pltpu.SemaphoreType.DMA((2, ITERS)),
            pltpu.SemaphoreType.DMA((2, ITERS)),
            pltpu.SemaphoreType.DMA((2, ITERS)),
        ],
        compiler_params=pltpu.CompilerParams(collective_id=0, has_side_effects=True),
    )(names, image_shift.transpose(2, 0, 1), names, window)
    return pl.pallas_call(
        functools.partial(untiling_kernel, tiles),
        out_shape=(out, out),
        in_specs=[vmem, vmem],
        out_specs=(vmem, vmem),
    )(found, inverse)


def solution(mesh):
    in_specs = (
        P(None, ("rep", "gx")),
        P(("rep", "gx")),
        P(None, ("rep", "gx")),
        P(("rep", "gx")),
        P(("rep", "gx"), None),
        P(None, ("rep", "gx"), None),
    )
    out_specs = (P(None, ("rep", "gx")), P(None, ("rep", "gx")))
    return jax.shard_map(
        on_device, mesh=mesh, in_specs=in_specs, out_specs=out_specs, check_vma=False
    )
```

```python
import functools

import jax
import jax.numpy as jnp
from jax import lax
from jax.experimental import pallas as pl
from jax.experimental.pallas import tpu as pltpu
from jax.sharding import PartitionSpec as P

ITERS = 4
MESH = pl.DeviceIdType.MESH
thole_factor = 0.39
LN2 = 0.6931471805599453
AWAY = 1e28
F32 = jnp.float32
BF16 = jnp.bfloat16


def split_two(value):
    high = value.astype(BF16)
    return high, (value - high.astype(F32)).astype(BF16)


def split_three(value):
    high = value.astype(BF16)
    rest = value - high.astype(F32)
    middle = rest.astype(BF16)
    return high, middle, (rest - middle.astype(F32)).astype(BF16)


def gather_tile(row, source, tiles):
    width = 128
    inner = jnp.broadcast_to(row & (width - 1), (8, width))
    outer = jnp.broadcast_to(row >> 7, (8, width))
    value = jnp.zeros((8, width), F32)
    for tile in range(tiles):
        picked = jnp.take_along_axis(
            source[pl.ds(tile * 8, 8), :], inner, axis=1, mode="promise_in_bounds"
        )
        value = jnp.where(outer == tile, picked, value)
    return value


def eight(index):
    return pl.ds(pl.multiple_of(index * 8, 8), 8)


def kernel(
    count,
    tiles,
    links,
    list_ref,
    shift_ref,
    names_ref,
    place_ref,
    polar_ref,
    field_ref,
    atom_ref,
    dip_ref,
    res_ref,
    feat,
    inverse,
    final,
    found_ref,
    window,
    middle,
    placed,
    centred,
    local,
    away,
    pair_own,
    pair_back,
    pair_left,
    bases,
    coefs,
    vectors,
    blocks,
    fields,
    summed,
    sent_p,
    ahead_p,
    sent_w,
    ahead_w,
    sent_f,
    back_f,
    dots,
    pack_sem,
    w_sem,
    f_sem,
    dot_sem,
):
    width = 128
    near = links - 1
    slots = near * tiles
    me = lax.axis_index("gx")
    after = lax.rem(me + 1, count)
    before = lax.rem(me + count - 1, count)

    barrier = pltpu.get_barrier_semaphore()

    def greet(step, carry):
        pl.semaphore_signal(
            barrier, inc=1, device_id={"gx": lax.rem(me + step, count)}, device_id_type=MESH
        )
        return carry

    lax.fori_loop(1, count, greet, 0)

    sub_ids = lax.broadcasted_iota(jnp.int32, (8, width), 0)
    low_rows = sub_ids < 4

    def strided(first, row):
        return pl.ds(first * 8 + row, tiles, stride=8)

    def grouped(size, body):
        def step(group, carry):
            for offset in range(size):
                body(group * size + offset)
            return carry

        lax.fori_loop(0, tiles // size, step, 0)

    for tile in range(tiles):
        lanes = pl.ds(tile * width, width)
        feat[tile * 8 : tile * 8 + 3, :] = place_ref[:, lanes]
        feat[tile * 8 + 3 : tile * 8 + 6, :] = field_ref[:, lanes]
        feat[tile * 8 + 6 : tile * 8 + 7, :] = polar_ref[:, lanes]
        feat[tile * 8 + 7 : tile * 8 + 8, :] = jnp.ones((1, width), F32)

    def fill(tile):
        value = gather_tile(atom_ref[pl.ds(tile, 1), :], feat, tiles)
        root = lax.rsqrt(value)
        window[eight(tile), :] = jnp.where(sub_ids == 7, pltpu.roll(root, 1, 0), value)

    grouped(8, fill)

    def copy_p():
        return pltpu.make_async_remote_copy(
            src_ref=sent_p,
            dst_ref=ahead_p,
            send_sem=pack_sem.at[0],
            recv_sem=pack_sem.at[1],
            device_id={"gx": before},
            device_id_type=MESH,
        )

    def copy_w(turn):
        return pltpu.make_async_remote_copy(
            src_ref=sent_w.at[turn],
            dst_ref=ahead_w.at[turn],
            send_sem=w_sem.at[0, turn],
            recv_sem=w_sem.at[1, turn],
            device_id={"gx": before},
            device_id_type=MESH,
        )

    pair_inputs = (0, 1, 2, 7)
    for at, row in enumerate(pair_inputs):
        sent_p[at] = window[strided(0, row), :]
    resid = [window[strided(0, 3 + axis), :] for axis in range(3)]
    for axis in range(3):
        sent_w[0, axis] = resid[axis]
    pl.semaphore_wait(barrier, count - 1)
    copy_p().start()
    copy_w(0).start()

    row_ids = lax.broadcasted_iota(jnp.int32, (width, width), 0)
    column_ids = lax.broadcasted_iota(jnp.int32, (width, width), 1)
    away[...] = jnp.where(row_ids == column_ids, AWAY, 0.0)

    def centre(first):
        whole = slice(first, first + tiles)
        ones = jnp.ones((tiles, width), F32)
        for axis in range(3):
            here = window[strided(first, axis), :]
            mean = jnp.floor(jnp.mean(here, axis=1, keepdims=True) + 0.5)
            mean = jnp.broadcast_to(mean, here.shape)
            middle[strided(first, axis), :] = mean
            here = here - mean
            local[axis, whole, :] = here
            bases[strided(first, axis), :] = here
            bases[strided(first, axis + 4), :] = here
        bases[strided(first, 3), :] = ones
        bases[strided(first, 7), :] = ones
        for row in range(3, 8):
            middle[strided(first, row), :] = jnp.zeros((tiles, width), F32)
        for tile in range(first, first + tiles):
            here = window[tile * 8 : tile * 8 + 8, :]
            root = jnp.broadcast_to(here[7:8, :], (8, width))
            placed[tile] = jnp.where(sub_ids < 3, here, jnp.where(sub_ids < 5, 0.0, root))
            centred[tile] = middle[tile * 8 : tile * 8 + 8, :]

    def split_rows(value):
        high = value.astype(BF16).astype(F32)
        rest = value - high
        middle = rest.astype(BF16).astype(F32)
        return high, middle, rest - middle

    def left_rows(tile):
        ones = jnp.ones((24, width), F32)
        return jnp.concatenate([*split_rows(placed[tile]), ones], axis=0).astype(BF16)

    def right_rows(other):
        high, mid, low = split_rows(jnp.where(sub_ids >= 5, other * -thole_factor, other))
        zero = jnp.zeros((8, width), F32)
        parts = []
        for axis in range(3):
            here = sub_ids == axis
            one = jnp.where(here, -1.0, 0.0)
            parts.append(
                [one, one, one] + [jnp.where(here, value, 0.0) for value in (high, mid, low)]
            )
        third = jnp.where(sub_ids == 7, high, 0.0)
        second = jnp.where(sub_ids == 6, mid, third)
        parts.append([jnp.where(sub_ids == 5, low, second), second, third, zero, zero, zero])
        parts = [jnp.concatenate(part, axis=0) for part in parts]
        return jnp.concatenate(parts, axis=1).astype(BF16)

    def offsets(left, right):
        return lax.dot_general(
            left, right, (((0,), (0,)), ((), ())), preferred_element_type=F32
        )

    def pair_rows(found, first, same):
        rows = slice(first, first + 16)
        off_x, off_y, off_z, scale = [
            found[rows, part * width : (part + 1) * width] for part in range(4)
        ]
        dist_sq = off_x * off_x + off_y * off_y + off_z * off_z
        if same:
            dist_sq = dist_sq + away[rows, :]
        inv = lax.rsqrt(dist_sq)
        inv_sq = inv * inv
        inv_cube = inv_sq * inv
        cube = dist_sq * (dist_sq * inv)
        decay = jnp.exp(scale * cube)
        three = inv_cube - inv_cube * decay
        five = inv_sq * (three + scale * decay)
        return three, five

    def store_pair(target, index, first, three, five):
        rows = slice(first, first + 16)
        more = slice(width + first, width + first + 16)
        high, low = split_two(five)
        target[index, rows, 0:width] = high
        target[index, rows, width : 2 * width] = low
        high, low = split_two(three)
        target[index, more, 0:width] = high
        target[index, more, width : 2 * width] = low

    def put_coefs(index, shift):
        def row(at):
            return jnp.broadcast_to(-shift[at : at + 1, :], (8, width))

        coefs[index, 0] = jnp.where(low_rows, row(0), 1.0)
        coefs[index, 1] = jnp.where(low_rows, row(1), row(2))
        coefs[index, 2] = shift

    def own_pairs(tile):
        here = placed[tile]
        found = offsets(left_rows(tile), right_rows(here))
        for first in range(0, width, 16):
            three, five = pair_rows(found, first, True)
            store_pair(pair_own, tile, first, three, five)
        put_coefs(tile, here - centred[tile])

    centre(0)
    grouped(8, own_pairs)

    lane_ids = row_ids
    tile_ids = lax.broadcasted_iota(jnp.int32, (tiles, width), 0)
    lane_row = lax.broadcasted_iota(jnp.int32, (tiles, width), 1).astype(F32)
    found_ref[...] = jnp.zeros_like(found_ref)

    def invert(tile):
        row = atom_ref[pl.ds(tile, 1), :]
        outer = tile_ids == (row >> 7)
        number = jnp.full((tiles, width), tile, jnp.int32).astype(F32)
        left = jnp.concatenate(
            [jnp.where(outer, number, 0.0), jnp.where(outer, lane_row, 0.0)], axis=0
        ).astype(BF16)
        right = jnp.where(lane_ids == (row & (width - 1)), 1.0, 0.0).astype(BF16)
        return lax.dot_general(
            left, right, (((1,), (1,)), ((), ())), preferred_element_type=F32
        )

    def invert_step(group, carry):
        total = found_ref[...]
        for offset in range(8):
            total = total + invert(group * 8 + offset)
        found_ref[...] = total
        return carry

    lax.fori_loop(0, tiles // 8, invert_step, 0)
    inverse[...] = (found_ref[:tiles] * float(width) + found_ref[tiles:]).astype(jnp.int32)

    copy_p().wait_recv()
    for at, row in enumerate(pair_inputs):
        window[strided(tiles, row), :] = ahead_p[at]
    centre(tiles)

    lengths = (jnp.where(me == count - 1, 4.0 * count, 0.0), 128.0, 2.0 * tiles)

    def far_pairs(tile):
        here = placed[tile]
        here_middle = centred[tile]
        left = left_rows(tile)
        for entry in range(near):
            slot = entry * tiles + tile
            named = list_ref[entry + 1, tile]
            crossing = jnp.full((8, width), named, jnp.int32) >= tiles
            moves = jnp.where(
                sub_ids == 0,
                jnp.where(crossing, lengths[0], 0.0),
                jnp.where(
                    sub_ids == 1,
                    shift_ref[entry + 1, 0, tile].astype(F32) * lengths[1],
                    jnp.where(sub_ids == 2, shift_ref[entry + 1, 1, tile].astype(F32) * lengths[2], 0.0),
                ),
            )
            other = placed[named] + moves
            put_coefs(tiles + slot, other - here_middle)
            put_coefs(tiles + slots + slot, here - (centred[named] + moves))
            found = offsets(left, right_rows(other))
            for first in range(0, width, 16):
                three, five = pair_rows(found, first, False)
                store_pair(pair_back, slot, first, three, five)
            for part in (slice(0, width), slice(width, 2 * width)):
                for half in (slice(0, width), slice(width, 2 * width)):
                    pair_left[slot, part, half] = pair_back[slot, part, half].T

    grouped(4, far_pairs)

    named_row = jnp.concatenate(
        [names_ref[entry + 1 : entry + 2, :] for entry in range(near)] * 3, axis=1
    )
    window_ids = lax.broadcasted_iota(jnp.int32, (2 * tiles, 3 * slots), 0)
    hits = jnp.where(window_ids == named_row, 1.0, 0.0).astype(BF16)

    alpha_inv = 1.0 / window[strided(0, 6), :]

    def put_vector(first, vec):
        whole = slice(first, first + tiles)
        along = local[0, whole, :] * vec[0] + local[1, whole, :] * vec[1] + local[2, whole, :] * vec[2]
        for axis in range(3):
            vectors[strided(first, axis), :] = 3.0 * vec[axis]
            vectors[strided(first, axis + 4), :] = -vec[axis]
        vectors[strided(first, 3), :] = 3.0 * along

    vectors[...] = jnp.zeros_like(vectors)

    def make_block(tile):
        base = bases[eight(tile), :]
        vec = vectors[eight(tile), :]

        def row(at):
            return jnp.broadcast_to(vec[at : at + 1, :], (8, width))

        moments = jnp.concatenate(
            [
                base * jnp.where(low_rows, row(0), row(3)),
                base * jnp.where(low_rows, row(1), row(2)),
            ],
            axis=0,
        )
        minus = jnp.concatenate([jnp.where(low_rows, 0.0, vec), jnp.zeros((8, width), F32)], axis=0)
        for part, value in enumerate(split_three(moments)):
            blocks[tile, part * 16 : part * 16 + 16, 0:width] = value
        for part, value in enumerate(split_three(minus)):
            blocks[tile, part * 16 : part * 16 + 16, width : 2 * width] = value

    def product(tile, weights, index):
        out = jnp.dot(blocks[tile], weights, preferred_element_type=F32)
        out = out[:, :width] + out[:, width:]
        out = (out[0:16] + out[16:32]) + out[32:48]
        total = coefs[index, 0] * out[0:8] + coefs[index, 1] * out[8:16]
        total = total + pltpu.roll(total, 4, 0)
        return total - coefs[index, 2] * jnp.broadcast_to(total[3:4, :], (8, width))

    def copy_f(turn):
        return pltpu.make_async_remote_copy(
            src_ref=sent_f.at[turn],
            dst_ref=back_f.at[turn],
            send_sem=f_sem.at[0, turn],
            recv_sem=f_sem.at[1, turn],
            device_id={"gx": after},
            device_id_type=MESH,
        )

    def back_step(tile):
        make_block(tile)
        for entry in range(near):
            slot = entry * tiles + tile
            fields[eight(slot), :] = product(tile, pair_back[slot], tiles + slot)

    def own_step(tile):
        summed[eight(tile), :] = product(tile, pair_own[tile], tile)

    def left_step(tile):
        total = summed[eight(tile), :]
        for entry in range(near):
            slot = entry * tiles + tile
            named = list_ref[entry + 1, tile]
            total = total + product(named, pair_left[slot], tiles + slots + slot)
        summed[eight(tile), :] = total

    def applied(turn, vec):
        put_vector(0, vec)
        grouped(16, back_step)
        back = jnp.concatenate(
            [fields[pl.ds(axis, slots, stride=8), :] for axis in range(3)], axis=1
        )
        spread = jnp.dot(
            hits, jnp.concatenate(split_three(back), axis=0), preferred_element_type=F32
        )
        for axis in range(3):
            sent_f[turn, axis] = spread[tiles:, axis * width : (axis + 1) * width]
        copy_f(turn).start()
        grouped(32, own_step)
        copy_w(turn).wait_recv()
        ahead = [ahead_w[turn, axis] for axis in range(3)]
        put_vector(tiles, ahead)
        for tile in range(tiles):
            make_block(tiles + tile)
        grouped(16, left_step)
        field = [
            summed[strided(0, axis), :] + spread[:tiles, axis * width : (axis + 1) * width]
            for axis in range(3)
        ]
        copy_f(turn).wait_recv()
        return [vec[axis] * alpha_inv - (field[axis] + back_f[turn, axis]) for axis in range(3)]

    def dot_rows(left, right):
        total = left[0] * right[0] + left[1] * right[1] + left[2] * right[2]
        return jnp.sum(total, axis=0, keepdims=True)

    def send_dots(turn, resid, w):
        dots[turn, 0] = jnp.where(
            sub_ids == 0, dot_rows(resid, resid), jnp.where(sub_ids == 1, dot_rows(resid, w), 0.0)
        )

        def send(step, carry):
            pltpu.make_async_remote_copy(
                src_ref=dots.at[turn, 0],
                dst_ref=dots.at[turn, step],
                send_sem=dot_sem.at[0, turn],
                recv_sem=dot_sem.at[1, turn],
                device_id={"gx": lax.rem(me + step, count)},
                device_id_type=MESH,
            ).start()
            return carry

        lax.fori_loop(1, count, send, 0)

    def wait_dots(turn, which):
        whole = dots.at[turn, pl.ds(1, count - 1)]
        pltpu.make_async_copy(whole, whole, dot_sem.at[which, turn]).wait()

    w = applied(0, resid)
    solution = direction = s = z = None
    norm_last = step_last = None
    for turn in range(ITERS):
        more_turns = turn + 1 < ITERS
        if more_turns:
            for axis in range(3):
                sent_w[turn + 1, axis] = w[axis]
            copy_w(turn + 1).start()
        send_dots(turn, resid, w)
        if more_turns:
            q = applied(turn + 1, w)
        wait_dots(turn, 1)
        sums = jnp.sum(jnp.sum(dots[turn], axis=0), axis=1, keepdims=True)
        norm = sums[0:1, :]
        product_now = sums[1:2, :]
        if turn == 0:
            step = norm / product_now
            direction, s = resid, w
            solution = [step * direction[axis] for axis in range(3)]
            if more_turns:
                z = q
        else:
            ratio = norm / norm_last
            step = norm / (product_now - ratio * norm / step_last)
            direction = [resid[axis] + ratio * direction[axis] for axis in range(3)]
            s = [w[axis] + ratio * s[axis] for axis in range(3)]
            solution = [solution[axis] + step * direction[axis] for axis in range(3)]
            if more_turns:
                z = [q[axis] + ratio * z[axis] for axis in range(3)]
        resid = [resid[axis] - step * s[axis] for axis in range(3)]
        if more_turns:
            w = [w[axis] - step * z[axis] for axis in range(3)]
        norm_last, step_last = norm, step

    for axis in range(3):
        final[strided(0, axis), :] = solution[axis]
        final[strided(0, 3 + axis), :] = resid[axis]

    def give(tile):
        value = gather_tile(inverse[pl.ds(tile, 1), :], final, tiles)
        lanes = pl.ds(pl.multiple_of(tile * width, width), width)
        dip_ref[:, lanes] = value[0:3]
        res_ref[:, lanes] = value[3:6]

    grouped(8, give)

    copy_p().wait_send()
    for turn in range(ITERS):
        copy_w(turn).wait_send()
        copy_f(turn).wait_send()
        wait_dots(turn, 0)


def on_device(positions, polar, field_ext, tile_atom, tile_list, image_shift):
    tiles, links = tile_list.shape
    atoms = tile_atom.shape[0]
    width = atoms // tiles
    near = links - 1
    count = lax.axis_size("gx")
    pairs = (2 * width, 2 * width)
    vmem = pl.BlockSpec(memory_space=pltpu.VMEM)
    smem = pl.BlockSpec(memory_space=pltpu.SMEM)
    out = jax.ShapeDtypeStruct((3, atoms), F32)
    vectors = pltpu.VMEM((ITERS, 3, tiles, width), F32)
    per_slab = pltpu.VMEM((tiles * 8, width), F32)
    per_window = pltpu.VMEM((2 * tiles * 8, width), F32)
    names = tile_list.T
    return pl.pallas_call(
        functools.partial(kernel, count, tiles, links),
        out_shape=(out, out),
        in_specs=[smem, smem, vmem, vmem, vmem, vmem, vmem],
        out_specs=(vmem, vmem),
        scratch_shapes=[
            per_slab,
            pltpu.VMEM((tiles, width), jnp.int32),
            per_slab,
            pltpu.VMEM((2 * tiles, width), F32),
            per_window,
            per_window,
            pltpu.VMEM((2 * tiles, 8, width), F32),
            pltpu.VMEM((2 * tiles, 8, width), F32),
            pltpu.VMEM((3, 2 * tiles, width), F32),
            pltpu.VMEM((width, width), F32),
            pltpu.VMEM((tiles,) + pairs, BF16),
            pltpu.VMEM((near * tiles,) + pairs, BF16),
            pltpu.VMEM((near * tiles,) + pairs, BF16),
            per_window,
            pltpu.VMEM(((1 + 2 * near) * tiles, 3, 8, width), F32),
            per_window,
            pltpu.VMEM((2 * tiles, 48, 2 * width), BF16),
            pltpu.VMEM((near * tiles * 8, width), F32),
            per_slab,
            pltpu.VMEM((4, tiles, width), F32),
            pltpu.VMEM((4, tiles, width), F32),
            vectors,
            vectors,
            vectors,
            vectors,
            pltpu.VMEM((ITERS, count, 8, width), F32),
            pltpu.SemaphoreType.DMA((2,)),
            pltpu.SemaphoreType.DMA((2, ITERS)),
            pltpu.SemaphoreType.DMA((2, ITERS)),
            pltpu.SemaphoreType.DMA((2, ITERS)),
        ],
        compiler_params=pltpu.CompilerParams(collective_id=0, has_side_effects=True),
    )(
        names,
        image_shift.transpose(2, 0, 1),
        names,
        positions,
        polar.reshape(1, atoms),
        field_ext,
        tile_atom.reshape(tiles, width),
    )


def solution(mesh):
    in_specs = (
        P(None, ("rep", "gx")),
        P(("rep", "gx")),
        P(None, ("rep", "gx")),
        P(("rep", "gx")),
        P(("rep", "gx"), None),
        P(None, ("rep", "gx"), None),
    )
    out_specs = (P(None, ("rep", "gx")), P(None, ("rep", "gx")))
    return jax.shard_map(
        on_device, mesh=mesh, in_specs=in_specs, out_specs=out_specs, check_vma=False
    )
```

```python
import functools

import jax
import jax.numpy as jnp
from jax import lax
from jax.experimental import pallas as pl
from jax.experimental.pallas import tpu as pltpu
from jax.sharding import PartitionSpec as P

ITERS = 4
MESH = pl.DeviceIdType.MESH
thole_factor = 0.39
LN2 = 0.6931471805599453
AWAY = 1e28
F32 = jnp.float32
BF16 = jnp.bfloat16


def split_two(value):
    high = value.astype(BF16)
    return high, (value - high.astype(F32)).astype(BF16)


def split_three(value):
    high = value.astype(BF16)
    rest = value - high.astype(F32)
    middle = rest.astype(BF16)
    return high, middle, (rest - middle.astype(F32)).astype(BF16)


def gather_tile(row, source, tiles, first=0):
    width = 128
    inner = jnp.broadcast_to(row & (width - 1), (8, width))
    outer = jnp.broadcast_to(row >> 7, (8, width))
    value = jnp.zeros((8, width), F32)
    for tile in range(tiles):
        picked = jnp.take_along_axis(
            source[pl.ds((first + tile) * 8, 8), :], inner, axis=1, mode="promise_in_bounds"
        )
        value = jnp.where(outer == tile, picked, value)
    return value


def eight(index):
    return pl.ds(pl.multiple_of(index * 8, 8), 8)


def kernel(
    count,
    tiles,
    links,
    list_ref,
    shift_ref,
    names_ref,
    place_ref,
    polar_ref,
    field_ref,
    atom_ref,
    dip_ref,
    res_ref,
    feat,
    inverse,
    final,
    found_ref,
    window,
    middle,
    placed,
    centred,
    local,
    away,
    pair_own,
    pair_back,
    pair_left,
    bases,
    coefs,
    vectors,
    blocks,
    fields,
    summed,
    sent_p,
    ahead_p,
    sent_w,
    ahead_w,
    sent_f,
    back_f,
    dots,
    pack_sem,
    w_sem,
    f_sem,
    dot_sem,
):
    width = 128
    near = links - 1
    slots = near * tiles
    me = lax.axis_index("gx")
    after = lax.rem(me + 1, count)
    before = lax.rem(me + count - 1, count)

    barrier = pltpu.get_barrier_semaphore()

    def greet(step, carry):
        pl.semaphore_signal(
            barrier, inc=1, device_id={"gx": lax.rem(me + step, count)}, device_id_type=MESH
        )
        return carry

    lax.fori_loop(1, count, greet, 0)

    sub_ids = lax.broadcasted_iota(jnp.int32, (8, width), 0)
    low_rows = sub_ids < 4

    def strided(first, row):
        return pl.ds(first * 8 + row, tiles, stride=8)

    def grouped(size, body):
        def step(group, carry):
            for offset in range(size):
                body(group * size + offset)
            return carry

        lax.fori_loop(0, tiles // size, step, 0)

    for tile in range(tiles):
        lanes = pl.ds(tile * width, width)
        feat[tile * 8 : tile * 8 + 3, :] = place_ref[:, lanes]
        feat[tile * 8 + 3 : tile * 8 + 6, :] = field_ref[:, lanes]
        feat[tile * 8 + 6 : tile * 8 + 7, :] = polar_ref[:, lanes]
        feat[tile * 8 + 7 : tile * 8 + 8, :] = jnp.ones((1, width), F32)

    def fill(tile):
        value = gather_tile(atom_ref[pl.ds(tile, 1), :], feat, tiles)
        root = lax.rsqrt(value)
        window[eight(tile), :] = jnp.where(sub_ids == 7, pltpu.roll(root, 1, 0), value)

    grouped(8, fill)

    def copy_p():
        return pltpu.make_async_remote_copy(
            src_ref=sent_p,
            dst_ref=ahead_p,
            send_sem=pack_sem.at[0],
            recv_sem=pack_sem.at[1],
            device_id={"gx": before},
            device_id_type=MESH,
        )

    def copy_w(turn):
        return pltpu.make_async_remote_copy(
            src_ref=sent_w.at[turn],
            dst_ref=ahead_w.at[turn],
            send_sem=w_sem.at[0, turn],
            recv_sem=w_sem.at[1, turn],
            device_id={"gx": before},
            device_id_type=MESH,
        )

    pair_inputs = (0, 1, 2, 7)
    for at, row in enumerate(pair_inputs):
        sent_p[at] = window[strided(0, row), :]
    resid = [window[strided(0, 3 + axis), :] for axis in range(3)]
    for axis in range(3):
        sent_w[0, axis] = resid[axis]
    pl.semaphore_wait(barrier, count - 1)
    copy_p().start()
    copy_w(0).start()

    row_ids = lax.broadcasted_iota(jnp.int32, (width, width), 0)
    column_ids = lax.broadcasted_iota(jnp.int32, (width, width), 1)
    away[...] = jnp.where(row_ids == column_ids, AWAY, 0.0)

    def centre(first):
        whole = slice(first, first + tiles)
        ones = jnp.ones((tiles, width), F32)
        for axis in range(3):
            here = window[strided(first, axis), :]
            mean = jnp.floor(jnp.mean(here, axis=1, keepdims=True) + 0.5)
            mean = jnp.broadcast_to(mean, here.shape)
            middle[strided(first, axis), :] = mean
            here = here - mean
            local[axis, whole, :] = here
            bases[strided(first, axis), :] = here
            bases[strided(first, axis + 4), :] = here
        bases[strided(first, 3), :] = ones
        bases[strided(first, 7), :] = ones
        for row in range(3, 8):
            middle[strided(first, row), :] = jnp.zeros((tiles, width), F32)
        for tile in range(first, first + tiles):
            here = window[tile * 8 : tile * 8 + 8, :]
            root = jnp.broadcast_to(here[7:8, :], (8, width))
            placed[tile] = jnp.where(sub_ids < 3, here, jnp.where(sub_ids < 5, 0.0, root))
            centred[tile] = middle[tile * 8 : tile * 8 + 8, :]

    def split_rows(value):
        high = value.astype(BF16).astype(F32)
        rest = value - high
        middle = rest.astype(BF16).astype(F32)
        return high, middle, rest - middle

    def left_rows(tile):
        ones = jnp.ones((24, width), F32)
        return jnp.concatenate([*split_rows(placed[tile]), ones], axis=0).astype(BF16)

    def right_rows(other):
        high, mid, low = split_rows(jnp.where(sub_ids >= 5, other * -thole_factor, other))
        zero = jnp.zeros((8, width), F32)
        parts = []
        for axis in range(3):
            here = sub_ids == axis
            one = jnp.where(here, -1.0, 0.0)
            parts.append(
                [one, one, one] + [jnp.where(here, value, 0.0) for value in (high, mid, low)]
            )
        third = jnp.where(sub_ids == 7, high, 0.0)
        second = jnp.where(sub_ids == 6, mid, third)
        parts.append([jnp.where(sub_ids == 5, low, second), second, third, zero, zero, zero])
        parts = [jnp.concatenate(part, axis=0) for part in parts]
        return jnp.concatenate(parts, axis=1).astype(BF16)

    def offsets(left, right):
        return lax.dot_general(
            left, right, (((0,), (0,)), ((), ())), preferred_element_type=F32
        )

    def pair_rows(found, first, same):
        rows = slice(first, first + 16)
        off_x, off_y, off_z, scale = [
            found[rows, part * width : (part + 1) * width] for part in range(4)
        ]
        dist_sq = off_x * off_x + off_y * off_y + off_z * off_z
        if same:
            dist_sq = dist_sq + away[rows, :]
        inv = lax.rsqrt(dist_sq)
        inv_sq = inv * inv
        inv_cube = inv_sq * inv
        cube = dist_sq * (dist_sq * inv)
        decay = jnp.exp(scale * cube)
        three = inv_cube - inv_cube * decay
        five = inv_sq * (three + scale * decay)
        return three, five

    def store_pair(target, index, first, three, five):
        for at, value in ((first, five), (width + first, three)):
            for half, part in enumerate(split_two(value)):
                target[index, at : at + 16, half * width : (half + 1) * width] = part

    def put_coefs(index, shift):
        def row(at):
            return jnp.broadcast_to(-shift[at : at + 1, :], (8, width))

        coefs[index, 0] = jnp.where(low_rows, row(0), 1.0)
        coefs[index, 1] = jnp.where(low_rows, row(1), row(2))
        coefs[index, 2] = shift

    def own_pairs(tile):
        here = placed[tile]
        found = offsets(left_rows(tile), right_rows(here))
        for first in range(0, width, 16):
            three, five = pair_rows(found, first, True)
            store_pair(pair_own, tile, first, three, five)
        put_coefs(tile, here - centred[tile])

    centre(0)
    grouped(8, own_pairs)

    lane_ids = row_ids
    tile_ids = lax.broadcasted_iota(jnp.int32, (tiles, width), 0)
    lane_row = lax.broadcasted_iota(jnp.int32, (tiles, width), 1).astype(F32)
    found_ref[...] = jnp.zeros_like(found_ref)

    def invert(tile):
        row = atom_ref[pl.ds(tile, 1), :]
        outer = tile_ids == (row >> 7)
        number = jnp.full((tiles, width), tile, jnp.int32).astype(F32)
        left = jnp.concatenate(
            [jnp.where(outer, number, 0.0), jnp.where(outer, lane_row, 0.0)], axis=0
        ).astype(BF16)
        right = jnp.where(lane_ids == (row & (width - 1)), 1.0, 0.0).astype(BF16)
        return lax.dot_general(
            left, right, (((1,), (1,)), ((), ())), preferred_element_type=F32
        )

    def invert_step(group, carry):
        total = found_ref[...]
        for offset in range(8):
            total = total + invert(group * 8 + offset)
        found_ref[...] = total
        return carry

    lax.fori_loop(0, tiles // 8, invert_step, 0)
    inverse[...] = (found_ref[:tiles] * float(width) + found_ref[tiles:]).astype(jnp.int32)

    copy_p().wait_recv()
    for at, row in enumerate(pair_inputs):
        window[strided(tiles, row), :] = ahead_p[at]
    centre(tiles)

    lengths = (jnp.where(me == count - 1, 4.0 * count, 0.0), 128.0, 2.0 * tiles)

    def far_pairs(tile):
        here = placed[tile]
        here_middle = centred[tile]
        left = left_rows(tile)
        for entry in range(near):
            slot = entry * tiles + tile
            named = list_ref[entry + 1, tile]
            crossing = jnp.full((8, width), named, jnp.int32) >= tiles
            moves = jnp.where(
                sub_ids == 0,
                jnp.where(crossing, lengths[0], 0.0),
                jnp.where(
                    sub_ids == 1,
                    shift_ref[entry + 1, 0, tile].astype(F32) * lengths[1],
                    jnp.where(sub_ids == 2, shift_ref[entry + 1, 1, tile].astype(F32) * lengths[2], 0.0),
                ),
            )
            other = placed[named] + moves
            put_coefs(tiles + slot, other - here_middle)
            put_coefs(tiles + slots + slot, here - (centred[named] + moves))
            found = offsets(left, right_rows(other))
            for first in range(0, width, 16):
                three, five = pair_rows(found, first, False)
                store_pair(pair_back, slot, first, three, five)
            for half in range(2):
                for part in (slice(0, width), slice(width, 2 * width)):
                    lanes = slice(half * width, (half + 1) * width)
                    pair_left[slot, part, lanes] = pair_back[slot, part, lanes].T


    named_row = jnp.concatenate(
        [names_ref[entry + 1 : entry + 2, :] for entry in range(near)] * 3, axis=1
    )
    window_ids = lax.broadcasted_iota(jnp.int32, (2 * tiles, 3 * slots), 0)
    hits = jnp.where(window_ids == named_row, 1.0, 0.0).astype(BF16)

    alpha_inv = 1.0 / window[strided(0, 6), :]

    def put_vector(first, vec):
        whole = slice(first, first + tiles)
        along = local[0, whole, :] * vec[0] + local[1, whole, :] * vec[1] + local[2, whole, :] * vec[2]
        for axis in range(3):
            vectors[strided(first, axis), :] = 3.0 * vec[axis]
            vectors[strided(first, axis + 4), :] = -vec[axis]
        vectors[strided(first, 3), :] = 3.0 * along

    vectors[...] = jnp.zeros_like(vectors)

    def make_block(tile):
        base = bases[eight(tile), :]
        vec = vectors[eight(tile), :]

        def row(at):
            return jnp.broadcast_to(vec[at : at + 1, :], (8, width))

        moments = jnp.concatenate(
            [
                base * jnp.where(low_rows, row(0), row(3)),
                base * jnp.where(low_rows, row(1), row(2)),
            ],
            axis=0,
        )
        minus = jnp.concatenate([jnp.where(low_rows, 0.0, vec), jnp.zeros((8, width), F32)], axis=0)
        for part, value in enumerate(split_three(moments)):
            blocks[tile, 0, part * 16 : part * 16 + 16, :] = value
        for part, value in enumerate(split_three(minus)):
            blocks[tile, 1, part * 16 : part * 16 + 16, :] = value

    def product(tile, pairs, slot, index):
        block = blocks[tile]
        weights = pairs[slot]
        out = jnp.dot(
            jnp.concatenate([block[0], block[1]], axis=1),
            weights,
            preferred_element_type=F32,
        )
        out = out[:, :width] + out[:, width:]
        out = (out[0:16] + out[16:32]) + out[32:48]
        total = coefs[index, 0] * out[0:8] + coefs[index, 1] * out[8:16]
        total = total + pltpu.roll(total, 4, 0)
        return total - coefs[index, 2] * jnp.broadcast_to(total[3:4, :], (8, width))

    def copy_f(turn):
        return pltpu.make_async_remote_copy(
            src_ref=sent_f.at[turn],
            dst_ref=back_f.at[turn],
            send_sem=f_sem.at[0, turn],
            recv_sem=f_sem.at[1, turn],
            device_id={"gx": after},
            device_id_type=MESH,
        )

    def back_step(tile):
        make_block(tile)
        for entry in range(near):
            slot = entry * tiles + tile
            fields[eight(slot), :] = product(tile, pair_back, slot, tiles + slot)

    def own_step(tile):
        summed[eight(tile), :] = product(tile, pair_own, tile, tile)

    def left_step(tile):
        total = summed[eight(tile), :]
        for entry in range(near):
            slot = entry * tiles + tile
            named = list_ref[entry + 1, tile]
            total = total + product(named, pair_left, slot, tiles + slots + slot)
        summed[eight(tile), :] = total

    put_vector(0, resid)

    def far_group(group, carry):
        for offset in range(4):
            back_step(lax.rem(group * 4 + offset + tiles - 4, tiles))
        for offset in range(4):
            far_pairs(group * 4 + offset)
        return carry

    lax.fori_loop(0, tiles // 4, far_group, 0)
    for offset in range(4):
        back_step(tiles - 4 + offset)

    def applied(turn, vec):
        if turn > 0:
            put_vector(0, vec)
            grouped(32, back_step)
        back = jnp.concatenate(
            [fields[pl.ds(axis, slots, stride=8), :] for axis in range(3)], axis=1
        )
        spread = jnp.dot(
            hits, jnp.concatenate(split_three(back), axis=0), preferred_element_type=F32
        )
        for axis in range(3):
            sent_f[turn, axis] = spread[tiles:, axis * width : (axis + 1) * width]
        copy_f(turn).start()
        grouped(32, own_step)
        copy_w(turn).wait_recv()
        ahead = [ahead_w[turn, axis] for axis in range(3)]
        put_vector(tiles, ahead)
        for tile in range(tiles):
            make_block(tiles + tile)
        grouped(32, left_step)
        field = [
            summed[strided(0, axis), :] + spread[:tiles, axis * width : (axis + 1) * width]
            for axis in range(3)
        ]
        copy_f(turn).wait_recv()
        return [vec[axis] * alpha_inv - (field[axis] + back_f[turn, axis]) for axis in range(3)]

    first_half = lax.broadcasted_iota(jnp.int32, (1, width), 1) < width // 2

    def dot_rows(left, right):
        total = left[0] * right[0] + left[1] * right[1] + left[2] * right[2]
        return jnp.sum(total, axis=0, keepdims=True)

    def send_dots(turn, resid, w):
        norm_row, product_row = dot_rows(resid, resid), dot_rows(resid, w)
        dots[turn, 0] = jnp.where(
            first_half,
            norm_row + pltpu.roll(norm_row, width // 2, 1),
            product_row + pltpu.roll(product_row, width // 2, 1),
        )

        def send(step, carry):
            pltpu.make_async_remote_copy(
                src_ref=dots.at[turn, 0],
                dst_ref=dots.at[turn, step],
                send_sem=dot_sem.at[0, turn],
                recv_sem=dot_sem.at[1, turn],
                device_id={"gx": lax.rem(me + step, count)},
                device_id_type=MESH,
            ).start()
            return carry

        lax.fori_loop(1, count, send, 0)

    def wait_dots(turn, which):
        whole = dots.at[turn, pl.ds(1, count - 1)]
        pltpu.make_async_copy(whole, whole, dot_sem.at[which, turn]).wait()

    def gather_last(solution, resid, direction, w, s):
        for axis in range(3):
            feat[strided(0, axis), :] = solution[axis]
            feat[strided(0, 3 + axis), :] = resid[axis]
            feat[strided(tiles, axis), :] = direction[axis]
            feat[strided(tiles, 3 + axis), :] = s[axis]
        for row, part in ((6, w[0]), (7, w[1]), (8 * tiles + 6, w[2])):
            feat[pl.ds(row, tiles, stride=8), :] = part

        feat[strided(tiles, 7), :] = w[2]

        def fetch(tile):
            row = inverse[pl.ds(tile, 1), :]
            final[eight(tile), :] = gather_tile(row, feat, tiles)
            final[eight(tiles + tile), :] = gather_tile(row, feat, tiles, tiles)

        grouped(4, fetch)

    w = applied(0, resid)
    solution = direction = s = z = None
    norm_last = step_last = None
    for turn in range(ITERS):
        more_turns = turn + 1 < ITERS
        if more_turns:
            for axis in range(3):
                sent_w[turn + 1, axis] = w[axis]
            copy_w(turn + 1).start()
        send_dots(turn, resid, w)
        if more_turns:
            q = applied(turn + 1, w)
        else:
            gather_last(solution, resid, direction, w, s)
        wait_dots(turn, 1)
        sums = jnp.sum(dots[turn], axis=0)
        norm = jnp.sum(jnp.where(first_half, sums, 0.0), axis=1, keepdims=True)
        product_now = jnp.sum(jnp.where(first_half, 0.0, sums), axis=1, keepdims=True)
        if turn == 0:
            step = norm / product_now
            direction, s = resid, w
            solution = [step * direction[axis] for axis in range(3)]
            if more_turns:
                z = q
        else:
            ratio = norm / norm_last
            step = norm / (product_now - ratio * norm / step_last)
            if not more_turns:
                break
            direction = [resid[axis] + ratio * direction[axis] for axis in range(3)]
            s = [w[axis] + ratio * s[axis] for axis in range(3)]
            solution = [solution[axis] + step * direction[axis] for axis in range(3)]
            if more_turns:
                z = [q[axis] + ratio * z[axis] for axis in range(3)]
        resid = [resid[axis] - step * s[axis] for axis in range(3)]
        if more_turns:
            w = [w[axis] - step * z[axis] for axis in range(3)]
        norm_last, step_last = norm, step

    plus = jnp.where(sub_ids < 3, 1.0, -1.0)
    by_ratio = plus * (step * ratio)
    by_step = plus * step

    def give(tile):
        first, second = final[eight(tile), :], final[eight(tiles + tile), :]
        third = jnp.where(sub_ids == 5, pltpu.roll(second, 7, 0), pltpu.roll(first, 5, 0))
        value = first + by_step * third + by_ratio * second
        lanes = pl.ds(pl.multiple_of(tile * width, width), width)
        dip_ref[:, lanes] = value[0:3]
        res_ref[:, lanes] = value[3:6]

    grouped(8, give)

    copy_p().wait_send()
    for turn in range(ITERS):
        copy_w(turn).wait_send()
        copy_f(turn).wait_send()
        wait_dots(turn, 0)


def on_device(positions, polar, field_ext, tile_atom, tile_list, image_shift):
    tiles, links = tile_list.shape
    atoms = tile_atom.shape[0]
    width = atoms // tiles
    near = links - 1
    count = lax.axis_size("gx")
    pairs = (2 * width, 2 * width)
    vmem = pl.BlockSpec(memory_space=pltpu.VMEM)
    smem = pl.BlockSpec(memory_space=pltpu.SMEM)
    out = jax.ShapeDtypeStruct((3, atoms), F32)
    vectors = pltpu.VMEM((ITERS, 3, tiles, width), F32)
    per_slab = pltpu.VMEM((tiles * 8, width), F32)
    per_window = pltpu.VMEM((2 * tiles * 8, width), F32)
    names = tile_list.T
    return pl.pallas_call(
        functools.partial(kernel, count, tiles, links),
        out_shape=(out, out),
        in_specs=[smem, smem, vmem, vmem, vmem, vmem, vmem],
        out_specs=(vmem, vmem),
        scratch_shapes=[
            per_window,
            pltpu.VMEM((tiles, width), jnp.int32),
            per_window,
            pltpu.VMEM((2 * tiles, width), F32),
            per_window,
            per_window,
            pltpu.VMEM((2 * tiles, 8, width), F32),
            pltpu.VMEM((2 * tiles, 8, width), F32),
            pltpu.VMEM((3, 2 * tiles, width), F32),
            pltpu.VMEM((width, width), F32),
            pltpu.VMEM((tiles,) + pairs, BF16),
            pltpu.VMEM((near * tiles,) + pairs, BF16),
            pltpu.VMEM((near * tiles,) + pairs, BF16),
            per_window,
            pltpu.VMEM(((1 + 2 * near) * tiles, 3, 8, width), F32),
            per_window,
            pltpu.VMEM((2 * tiles, 2, 48, width), BF16),
            pltpu.VMEM((near * tiles * 8, width), F32),
            per_slab,
            pltpu.VMEM((4, tiles, width), F32),
            pltpu.VMEM((4, tiles, width), F32),
            vectors,
            vectors,
            vectors,
            vectors,
            pltpu.VMEM((ITERS, count, 1, width), F32),
            pltpu.SemaphoreType.DMA((2,)),
            pltpu.SemaphoreType.DMA((2, ITERS)),
            pltpu.SemaphoreType.DMA((2, ITERS)),
            pltpu.SemaphoreType.DMA((2, ITERS)),
        ],
        compiler_params=pltpu.CompilerParams(collective_id=0, has_side_effects=True),
    )(
        names,
        image_shift.transpose(2, 0, 1),
        names,
        positions,
        polar.reshape(1, atoms),
        field_ext,
        tile_atom.reshape(tiles, width),
    )


def solution(mesh):
    in_specs = (
        P(None, ("rep", "gx")),
        P(("rep", "gx")),
        P(None, ("rep", "gx")),
        P(("rep", "gx")),
        P(("rep", "gx"), None),
        P(None, ("rep", "gx"), None),
    )
    out_specs = (P(None, ("rep", "gx")), P(None, ("rep", "gx")))
    return jax.shard_map(
        on_device, mesh=mesh, in_specs=in_specs, out_specs=out_specs, check_vma=False
    )
```

```python
import functools

import jax
import jax.numpy as jnp
from jax import lax
from jax.experimental import pallas as pl
from jax.experimental.pallas import tpu as pltpu
from jax.sharding import PartitionSpec as P

ITERS = 4
FAR = 4
MESH = pl.DeviceIdType.MESH
thole_factor = 0.39
LN2 = 0.6931471805599453
AWAY = 1e28
F32 = jnp.float32
BF16 = jnp.bfloat16


def split_two(value):
    high = value.astype(BF16)
    return high, (value - high.astype(F32)).astype(BF16)


def split_three(value):
    high = value.astype(BF16)
    rest = value - high.astype(F32)
    middle = rest.astype(BF16)
    return high, middle, (rest - middle.astype(F32)).astype(BF16)


def gather_tile(row, source, tiles, first=0):
    width = 128
    inner = jnp.broadcast_to(row & (width - 1), (8, width))
    outer = jnp.broadcast_to(row >> 7, (8, width))
    value = jnp.zeros((8, width), F32)
    for tile in range(tiles):
        picked = jnp.take_along_axis(
            source[pl.ds((first + tile) * 8, 8), :], inner, axis=1, mode="promise_in_bounds"
        )
        value = jnp.where(outer == tile, picked, value)
    return value


def eight(index):
    return pl.ds(pl.multiple_of(index * 8, 8), 8)


def kernel(
    count,
    tiles,
    links,
    list_ref,
    shift_ref,
    names_ref,
    place_ref,
    polar_ref,
    field_ref,
    atom_ref,
    out_ref,
    feat,
    inverse,
    final,
    found_ref,
    window,
    middle,
    placed,
    centred,
    local,
    away,
    pair_own,
    pair_back,
    pair_left,
    bases,
    coefs,
    vectors,
    blocks,
    fields,
    summed,
    sent_p,
    ahead_p,
    sent_w,
    ahead_w,
    sent_f,
    back_f,
    dots,
    pack_sem,
    w_sem,
    f_sem,
    dot_sem,
):
    width = 128
    near = links - 1
    slots = near * tiles
    me = lax.axis_index("gx")
    after = lax.rem(me + 1, count)
    before = lax.rem(me + count - 1, count)

    barrier = pltpu.get_barrier_semaphore()

    def greet(step, carry):
        pl.semaphore_signal(
            barrier, inc=1, device_id={"gx": lax.rem(me + step, count)}, device_id_type=MESH
        )
        return carry

    lax.fori_loop(1, count, greet, 0)

    sub_ids = lax.broadcasted_iota(jnp.int32, (8, width), 0)
    low_rows = sub_ids < 4

    def strided(first, row):
        return pl.ds(first * 8 + row, tiles, stride=8)

    def grouped(size, body):
        def step(group, carry):
            for offset in range(size):
                body(group * size + offset)
            return carry

        lax.fori_loop(0, tiles // size, step, 0)

    for tile in range(tiles):
        lanes = pl.ds(tile * width, width)
        feat[tile * 8 : tile * 8 + 3, :] = place_ref[:, lanes]
        feat[tile * 8 + 3 : tile * 8 + 6, :] = field_ref[:, lanes]
        feat[tile * 8 + 6 : tile * 8 + 7, :] = polar_ref[:, lanes]
        feat[tile * 8 + 7 : tile * 8 + 8, :] = jnp.ones((1, width), F32)

    def fill(tile):
        value = gather_tile(atom_ref[pl.ds(tile, 1), :], feat, tiles)
        root = lax.rsqrt(value)
        window[eight(tile), :] = jnp.where(sub_ids == 7, pltpu.roll(root, 1, 0), value)

    grouped(8, fill)

    def copy_p():
        return pltpu.make_async_remote_copy(
            src_ref=sent_p,
            dst_ref=ahead_p,
            send_sem=pack_sem.at[0],
            recv_sem=pack_sem.at[1],
            device_id={"gx": before},
            device_id_type=MESH,
        )

    def copy_w(turn):
        return pltpu.make_async_remote_copy(
            src_ref=sent_w.at[turn],
            dst_ref=ahead_w.at[turn],
            send_sem=w_sem.at[0, turn],
            recv_sem=w_sem.at[1, turn],
            device_id={"gx": before},
            device_id_type=MESH,
        )

    pair_inputs = (0, 1, 2, 7)
    for at, row in enumerate(pair_inputs):
        sent_p[at] = window[strided(0, row), :]
    resid = [window[strided(0, 3 + axis), :] for axis in range(3)]
    for axis in range(3):
        sent_w[0, axis] = resid[axis]
    pl.semaphore_wait(barrier, count - 1)
    copy_p().start()
    copy_w(0).start()

    row_ids = lax.broadcasted_iota(jnp.int32, (width, width), 0)
    column_ids = lax.broadcasted_iota(jnp.int32, (width, width), 1)
    away[...] = jnp.where(row_ids == column_ids, AWAY, 0.0)

    def centre(first):
        whole = slice(first, first + tiles)
        ones = jnp.ones((tiles, width), F32)
        for axis in range(3):
            here = window[strided(first, axis), :]
            mean = jnp.floor(jnp.mean(here, axis=1, keepdims=True) + 0.5)
            mean = jnp.broadcast_to(mean, here.shape)
            middle[strided(first, axis), :] = mean
            here = here - mean
            local[axis, whole, :] = here
            bases[strided(first, axis), :] = here
            bases[strided(first, axis + 4), :] = here
        bases[strided(first, 3), :] = ones
        bases[strided(first, 7), :] = ones
        for row in range(3, 8):
            middle[strided(first, row), :] = jnp.zeros((tiles, width), F32)
        for tile in range(first, first + tiles):
            here = window[tile * 8 : tile * 8 + 8, :]
            root = jnp.broadcast_to(here[7:8, :], (8, width))
            placed[tile] = jnp.where(sub_ids < 3, here, jnp.where(sub_ids < 5, 0.0, root))
            centred[tile] = middle[tile * 8 : tile * 8 + 8, :]

    def split_rows(value):
        high = value.astype(BF16).astype(F32)
        rest = value - high
        middle = rest.astype(BF16).astype(F32)
        return high, middle, rest - middle

    def left_rows(tile):
        ones = jnp.ones((24, width), F32)
        return jnp.concatenate([*split_rows(placed[tile]), ones], axis=0).astype(BF16)

    def right_rows(other):
        high, mid, low = split_rows(jnp.where(sub_ids >= 5, other * -thole_factor, other))
        zero = jnp.zeros((8, width), F32)
        parts = []
        for axis in range(3):
            here = sub_ids == axis
            one = jnp.where(here, -1.0, 0.0)
            parts.append(
                [one, one, one] + [jnp.where(here, value, 0.0) for value in (high, mid, low)]
            )
        third = jnp.where(sub_ids == 7, high, 0.0)
        second = jnp.where(sub_ids == 6, mid, third)
        parts.append([jnp.where(sub_ids == 5, low, second), second, third, zero, zero, zero])
        parts = [jnp.concatenate(part, axis=0) for part in parts]
        return jnp.concatenate(parts, axis=1).astype(BF16)

    def offsets(left, right):
        return lax.dot_general(
            left, right, (((0,), (0,)), ((), ())), preferred_element_type=F32
        )

    def pair_rows(found, first, same):
        rows = slice(first, first + 16)
        off_x, off_y, off_z, scale = [
            found[rows, part * width : (part + 1) * width] for part in range(4)
        ]
        dist_sq = off_x * off_x + off_y * off_y + off_z * off_z
        if same:
            dist_sq = dist_sq + away[rows, :]
        inv = lax.rsqrt(dist_sq)
        inv_sq = inv * inv
        inv_cube = inv_sq * inv
        cube = dist_sq * (dist_sq * inv)
        decay = jnp.exp(scale * cube)
        three = inv_cube - inv_cube * decay
        five = inv_sq * (three + scale * decay)
        return three, five

    def store_pair(target, index, first, three, five):
        for at, value in ((first, five), (width + first, three)):
            for half, part in enumerate(split_two(value)):
                target[index, at : at + 16, half * width : (half + 1) * width] = part

    def put_coefs(index, shift):
        def row(at):
            return jnp.broadcast_to(-shift[at : at + 1, :], (8, width))

        coefs[index, 0] = jnp.where(low_rows, row(0), 1.0)
        coefs[index, 1] = jnp.where(low_rows, row(1), row(2))
        coefs[index, 2] = shift

    def own_pairs(tile):
        here = placed[tile]
        found = offsets(left_rows(tile), right_rows(here))
        for first in range(0, width, 16):
            three, five = pair_rows(found, first, True)
            store_pair(pair_own, tile, first, three, five)
        put_coefs(tile, here - centred[tile])

    centre(0)
    grouped(8, own_pairs)

    lane_ids = row_ids
    tile_ids = lax.broadcasted_iota(jnp.int32, (tiles, width), 0)
    lane_row = lax.broadcasted_iota(jnp.int32, (tiles, width), 1).astype(F32)
    found_ref[...] = jnp.zeros_like(found_ref)

    def invert(tile):
        row = atom_ref[pl.ds(tile, 1), :]
        outer = tile_ids == (row >> 7)
        number = jnp.full((tiles, width), tile, jnp.int32).astype(F32)
        left = jnp.concatenate(
            [jnp.where(outer, number, 0.0), jnp.where(outer, lane_row, 0.0)], axis=0
        ).astype(BF16)
        right = jnp.where(lane_ids == (row & (width - 1)), 1.0, 0.0).astype(BF16)
        return lax.dot_general(
            left, right, (((1,), (1,)), ((), ())), preferred_element_type=F32
        )

    def invert_step(group, carry):
        total = found_ref[...]
        for offset in range(8):
            total = total + invert(group * 8 + offset)
        found_ref[...] = total
        return carry

    lax.fori_loop(0, tiles // 8, invert_step, 0)
    inverse[...] = (found_ref[:tiles] * float(width) + found_ref[tiles:]).astype(jnp.int32)

    copy_p().wait_recv()
    for at, row in enumerate(pair_inputs):
        window[strided(tiles, row), :] = ahead_p[at]
    centre(tiles)

    lengths = (jnp.where(me == count - 1, 4.0 * count, 0.0), 128.0, 2.0 * tiles)

    def far_pairs(tile):
        here = placed[tile]
        here_middle = centred[tile]
        left = left_rows(tile)
        for entry in range(near):
            slot = entry * tiles + tile
            named = list_ref[entry + 1, tile]
            crossing = jnp.full((8, width), named, jnp.int32) >= tiles
            moves = jnp.where(
                sub_ids == 0,
                jnp.where(crossing, lengths[0], 0.0),
                jnp.where(
                    sub_ids == 1,
                    shift_ref[entry + 1, 0, tile].astype(F32) * lengths[1],
                    jnp.where(sub_ids == 2, shift_ref[entry + 1, 1, tile].astype(F32) * lengths[2], 0.0),
                ),
            )
            other = placed[named] + moves
            put_coefs(tiles + slot, other - here_middle)
            put_coefs(tiles + slots + slot, here - (centred[named] + moves))
            found = offsets(left, right_rows(other))
            for first in range(0, width, 16):
                three, five = pair_rows(found, first, False)
                store_pair(pair_back, slot, first, three, five)
            for half in range(2):
                for part in (slice(0, width), slice(width, 2 * width)):
                    lanes = slice(half * width, (half + 1) * width)
                    pair_left[slot, part, lanes] = pair_back[slot, part, lanes].T


    named_row = jnp.concatenate(
        [names_ref[entry + 1 : entry + 2, :] for entry in range(near)] * 3, axis=1
    )
    window_ids = lax.broadcasted_iota(jnp.int32, (2 * tiles, 3 * slots), 0)
    hits = jnp.where(window_ids == named_row, 1.0, 0.0).astype(BF16)

    alpha_inv = 1.0 / window[strided(0, 6), :]

    def put_vector(first, vec):
        whole = slice(first, first + tiles)
        along = local[0, whole, :] * vec[0] + local[1, whole, :] * vec[1] + local[2, whole, :] * vec[2]
        for axis in range(3):
            vectors[strided(first, axis), :] = 3.0 * vec[axis]
            vectors[strided(first, axis + 4), :] = -vec[axis]
        vectors[strided(first, 3), :] = 3.0 * along

    vectors[...] = jnp.zeros_like(vectors)

    def make_block(tile):
        base = bases[eight(tile), :]
        vec = vectors[eight(tile), :]

        def row(at):
            return jnp.broadcast_to(vec[at : at + 1, :], (8, width))

        moments = jnp.concatenate(
            [
                base * jnp.where(low_rows, row(0), row(3)),
                base * jnp.where(low_rows, row(1), row(2)),
            ],
            axis=0,
        )
        minus = jnp.concatenate([jnp.where(low_rows, 0.0, vec), jnp.zeros((8, width), F32)], axis=0)
        for part, value in enumerate(split_three(moments)):
            blocks[tile, 0, part * 16 : part * 16 + 16, :] = value
        for part, value in enumerate(split_three(minus)):
            blocks[tile, 1, part * 16 : part * 16 + 16, :] = value

    def product(tile, pairs, slot, index):
        block = blocks[tile]
        weights = pairs[slot]
        out = jnp.dot(
            jnp.concatenate([block[0], block[1]], axis=1),
            weights,
            preferred_element_type=F32,
        )
        out = out[:, :width] + out[:, width:]
        out = (out[0:16] + out[16:32]) + out[32:48]
        total = coefs[index, 0] * out[0:8] + coefs[index, 1] * out[8:16]
        total = total + pltpu.roll(total, 4, 0)
        return total - coefs[index, 2] * jnp.broadcast_to(total[3:4, :], (8, width))

    def copy_f(turn):
        return pltpu.make_async_remote_copy(
            src_ref=sent_f.at[turn],
            dst_ref=back_f.at[turn],
            send_sem=f_sem.at[0, turn],
            recv_sem=f_sem.at[1, turn],
            device_id={"gx": after},
            device_id_type=MESH,
        )

    def back_step(tile):
        make_block(tile)
        for entry in range(near):
            slot = entry * tiles + tile
            fields[eight(slot), :] = product(tile, pair_back, slot, tiles + slot)

    def own_step(tile):
        summed[eight(tile), :] = product(tile, pair_own, tile, tile)

    def left_step(tile):
        total = summed[eight(tile), :]
        for entry in range(near):
            slot = entry * tiles + tile
            named = list_ref[entry + 1, tile]
            total = total + product(named, pair_left, slot, tiles + slots + slot)
        summed[eight(tile), :] = total

    put_vector(0, resid)

    def far_group(group, carry):
        for offset in range(FAR):
            back_step(lax.rem(group * FAR + offset + tiles - FAR, tiles))
        for offset in range(FAR):
            far_pairs(group * FAR + offset)
        return carry

    lax.fori_loop(0, tiles // FAR, far_group, 0)
    for offset in range(FAR):
        back_step(tiles - FAR + offset)

    def applied(turn, vec, meanwhile=None):
        if turn > 0:
            put_vector(0, vec)
            grouped(32, back_step)
        back = jnp.concatenate(
            [fields[pl.ds(axis, slots, stride=8), :] for axis in range(3)], axis=1
        )
        spread = jnp.dot(
            hits, jnp.concatenate(split_three(back), axis=0), preferred_element_type=F32
        )
        for axis in range(3):
            sent_f[turn, axis] = spread[tiles:, axis * width : (axis + 1) * width]
        copy_f(turn).start()
        if meanwhile is not None:
            meanwhile()
        grouped(32, own_step)
        copy_w(turn).wait_recv()
        ahead = [ahead_w[turn, axis] for axis in range(3)]
        put_vector(tiles, ahead)
        for tile in range(tiles):
            make_block(tiles + tile)
        grouped(32, left_step)
        field = [
            summed[strided(0, axis), :] + spread[:tiles, axis * width : (axis + 1) * width]
            for axis in range(3)
        ]
        return [vec[axis] * alpha_inv - field[axis] for axis in range(3)]

    first_half = lax.broadcasted_iota(jnp.int32, (1, width), 1) < width // 2

    def dot_rows(left, right):
        total = left[0] * right[0] + left[1] * right[1] + left[2] * right[2]
        return jnp.sum(total, axis=0, keepdims=True)

    def send_dots(turn, resid, w):
        norm_row, product_row = dot_rows(resid, resid), dot_rows(resid, w)
        dots[turn, 0] = jnp.where(
            first_half,
            norm_row + pltpu.roll(norm_row, width // 2, 1),
            product_row + pltpu.roll(product_row, width // 2, 1),
        )

        def send(step, carry):
            pltpu.make_async_remote_copy(
                src_ref=dots.at[turn, 0],
                dst_ref=dots.at[turn, step],
                send_sem=dot_sem.at[0, turn],
                recv_sem=dot_sem.at[1, turn],
                device_id={"gx": lax.rem(me + step, count)},
                device_id_type=MESH,
            ).start()
            return carry

        lax.fori_loop(1, count, send, 0)

    def wait_dots(turn, which):
        whole = dots.at[turn, pl.ds(1, count - 1)]
        pltpu.make_async_copy(whole, whole, dot_sem.at[which, turn]).wait()

    def gather_last(solution, resid, direction, w, s):
        for axis in range(3):
            feat[strided(0, axis), :] = solution[axis]
            feat[strided(0, 3 + axis), :] = resid[axis]
            feat[strided(tiles, axis), :] = direction[axis]
            feat[strided(tiles, 3 + axis), :] = s[axis]
        for row, part in ((6, w[0]), (7, w[1]), (8 * tiles + 6, w[2])):
            feat[pl.ds(row, tiles, stride=8), :] = part

        feat[strided(tiles, 7), :] = w[2]

        def fetch(tile):
            row = inverse[pl.ds(tile, 1), :]
            final[eight(tile), :] = gather_tile(row, feat, tiles)
            final[eight(tiles + tile), :] = gather_tile(row, feat, tiles, tiles)

        grouped(4, fetch)

    w = applied(0, resid)
    copy_f(0).wait_recv()
    w = [w[axis] - back_f[0, axis] for axis in range(3)]
    solution = direction = s = z = None
    norm_last = step_last = None
    for turn in range(ITERS):
        more_turns = turn + 1 < ITERS
        if more_turns:
            for axis in range(3):
                sent_w[turn + 1, axis] = w[axis]
            copy_w(turn + 1).start()
            send_dots(turn, resid, w)
            q = applied(turn + 1, w)
        else:
            send_dots(turn, resid, w)
            gather_last(solution, resid, direction, w, s)
        wait_dots(turn, 1)
        sums = jnp.sum(dots[turn], axis=0)
        norm = jnp.sum(jnp.where(first_half, sums, 0.0), axis=1, keepdims=True)
        product_now = jnp.sum(jnp.where(first_half, 0.0, sums), axis=1, keepdims=True)
        if turn == 0:
            step = norm / product_now
            direction, s = resid, w
            solution = [step * direction[axis] for axis in range(3)]
            if more_turns:
                z = q
        else:
            ratio = norm / norm_last
            step = norm / (product_now - ratio * norm / step_last)
            if not more_turns:
                break
            direction = [resid[axis] + ratio * direction[axis] for axis in range(3)]
            s = [w[axis] + ratio * s[axis] for axis in range(3)]
            solution = [solution[axis] + step * direction[axis] for axis in range(3)]
            z = [q[axis] + ratio * z[axis] for axis in range(3)]
        resid = [resid[axis] - step * s[axis] for axis in range(3)]
        if more_turns:
            w = [w[axis] - step * z[axis] for axis in range(3)]
            copy_f(turn + 1).wait_recv()
            late = [back_f[turn + 1, axis] for axis in range(3)]
            w = [w[axis] + step * late[axis] for axis in range(3)]
            z = [z[axis] - late[axis] for axis in range(3)]
        norm_last, step_last = norm, step

    plus = jnp.where(sub_ids < 3, 1.0, -1.0)
    by_ratio = plus * (step * ratio)
    by_step = plus * step

    def give(tile):
        first, second = final[eight(tile), :], final[eight(tiles + tile), :]
        third = jnp.where(sub_ids == 5, pltpu.roll(second, 7, 0), pltpu.roll(first, 5, 0))
        value = first + by_step * third + by_ratio * second
        lanes = pl.ds(pl.multiple_of(tile * width, width), width)
        out_ref[:, lanes] = value[0:6]

    grouped(8, give)

    copy_p().wait_send()
    for turn in range(ITERS):
        copy_w(turn).wait_send()
        copy_f(turn).wait_send()
        wait_dots(turn, 0)


def on_device(positions, polar, field_ext, tile_atom, tile_list, image_shift):
    tiles, links = tile_list.shape
    atoms = tile_atom.shape[0]
    width = atoms // tiles
    near = links - 1
    count = lax.axis_size("gx")
    pairs = (2 * width, 2 * width)
    vmem = pl.BlockSpec(memory_space=pltpu.VMEM)
    smem = pl.BlockSpec(memory_space=pltpu.SMEM)
    out = jax.ShapeDtypeStruct((6, atoms), F32)
    vectors = pltpu.VMEM((ITERS, 3, tiles, width), F32)
    per_slab = pltpu.VMEM((tiles * 8, width), F32)
    per_window = pltpu.VMEM((2 * tiles * 8, width), F32)
    names = tile_list.T
    both = pl.pallas_call(
        functools.partial(kernel, count, tiles, links),
        out_shape=out,
        in_specs=[smem, smem, vmem, vmem, vmem, vmem, vmem],
        out_specs=vmem,
        scratch_shapes=[
            per_window,
            pltpu.VMEM((tiles, width), jnp.int32),
            per_window,
            pltpu.VMEM((2 * tiles, width), F32),
            per_window,
            per_window,
            pltpu.VMEM((2 * tiles, 8, width), F32),
            pltpu.VMEM((2 * tiles, 8, width), F32),
            pltpu.VMEM((3, 2 * tiles, width), F32),
            pltpu.VMEM((width, width), F32),
            pltpu.VMEM((tiles,) + pairs, BF16),
            pltpu.VMEM((near * tiles,) + pairs, BF16),
            pltpu.VMEM((near * tiles,) + pairs, BF16),
            per_window,
            pltpu.VMEM(((1 + 2 * near) * tiles, 3, 8, width), F32),
            per_window,
            pltpu.VMEM((2 * tiles, 2, 48, width), BF16),
            pltpu.VMEM((near * tiles * 8, width), F32),
            per_slab,
            pltpu.VMEM((4, tiles, width), F32),
            pltpu.VMEM((4, tiles, width), F32),
            vectors,
            vectors,
            vectors,
            vectors,
            pltpu.VMEM((ITERS, count, 1, width), F32),
            pltpu.SemaphoreType.DMA((2,)),
            pltpu.SemaphoreType.DMA((2, ITERS)),
            pltpu.SemaphoreType.DMA((2, ITERS)),
            pltpu.SemaphoreType.DMA((2, ITERS)),
        ],
        compiler_params=pltpu.CompilerParams(collective_id=0, has_side_effects=True),
    )(
        names,
        image_shift.transpose(2, 0, 1),
        names,
        positions,
        polar.reshape(1, atoms),
        field_ext,
        tile_atom.reshape(tiles, width),
    )
    return both[:3], both[3:]


def solution(mesh):
    in_specs = (
        P(None, ("rep", "gx")),
        P(("rep", "gx")),
        P(None, ("rep", "gx")),
        P(("rep", "gx")),
        P(("rep", "gx"), None),
        P(None, ("rep", "gx"), None),
    )
    out_specs = (P(None, ("rep", "gx")), P(None, ("rep", "gx")))
    return jax.shard_map(
        on_device, mesh=mesh, in_specs=in_specs, out_specs=out_specs, check_vma=False
    )
```

```python
import functools

import jax
import jax.numpy as jnp
from jax import lax
from jax.experimental import pallas as pl
from jax.experimental.pallas import tpu as pltpu
from jax.sharding import PartitionSpec as P

ITERS = 4
FAR = 4
MESH = pl.DeviceIdType.MESH
thole_factor = 0.39
LN2 = 0.6931471805599453
AWAY = 1e28
F32 = jnp.float32
BF16 = jnp.bfloat16


def split_two(value):
    high = value.astype(BF16)
    return high, (value - high.astype(F32)).astype(BF16)


def split_three(value):
    high = value.astype(BF16)
    rest = value - high.astype(F32)
    middle = rest.astype(BF16)
    return high, middle, (rest - middle.astype(F32)).astype(BF16)


def gather_tile(row, source, tiles, first=0):
    width = 128
    inner = jnp.broadcast_to(row & (width - 1), (8, width))
    outer = jnp.broadcast_to(row >> 7, (8, width))
    value = jnp.zeros((8, width), F32)
    for tile in range(tiles):
        picked = jnp.take_along_axis(
            source[pl.ds((first + tile) * 8, 8), :], inner, axis=1, mode="promise_in_bounds"
        )
        value = jnp.where(outer == tile, picked, value)
    return value


def eight(index):
    return pl.ds(pl.multiple_of(index * 8, 8), 8)


def kernel(
    count,
    tiles,
    links,
    list_hbm,
    shift_hbm,
    place_hbm,
    polar_hbm,
    field_hbm,
    atom_hbm,
    out_any,
    list_ref,
    shift_ref,
    names_ref,
    place_ref,
    polar_ref,
    field_ref,
    atom_ref,
    out_ref,
    in_sem,
    out_sem,
    feat,
    inverse,
    final,
    found_ref,
    window,
    middle,
    placed,
    centred,
    local,
    away,
    pair_own,
    pair_back,
    pair_left,
    bases,
    coefs,
    vectors,
    blocks,
    fields,
    summed,
    sent_p,
    ahead_p,
    sent_w,
    ahead_w,
    sent_f,
    back_f,
    dots,
    pack_sem,
    w_sem,
    f_sem,
    dot_sem,
):
    width = 128
    near = links - 1
    slots = near * tiles
    me = lax.axis_index("gx")
    after = lax.rem(me + 1, count)
    before = lax.rem(me + count - 1, count)

    arrivals = [
        pltpu.make_async_copy(source, target, in_sem.at[at])
        for at, (source, target) in enumerate(
            (
                (place_hbm, place_ref),
                (field_hbm, field_ref),
                (polar_hbm, polar_ref),
                (atom_hbm, atom_ref),
                (list_hbm, list_ref),
                (shift_hbm, shift_ref),
                (list_hbm, names_ref),
            )
        )
    ]
    for arrival in arrivals:
        arrival.start()

    barrier = pltpu.get_barrier_semaphore()

    def greet(step, carry):
        pl.semaphore_signal(
            barrier, inc=1, device_id={"gx": lax.rem(me + step, count)}, device_id_type=MESH
        )
        return carry

    lax.fori_loop(1, count, greet, 0)

    sub_ids = lax.broadcasted_iota(jnp.int32, (8, width), 0)
    low_rows = sub_ids < 4

    def strided(first, row):
        return pl.ds(first * 8 + row, tiles, stride=8)

    def grouped(size, body):
        def step(group, carry):
            for offset in range(size):
                body(group * size + offset)
            return carry

        lax.fori_loop(0, tiles // size, step, 0)

    for arrival in arrivals[:4]:
        arrival.wait()
    for tile in range(tiles):
        lanes = pl.ds(tile * width, width)
        feat[tile * 8 : tile * 8 + 3, :] = place_ref[:, lanes]
        feat[tile * 8 + 3 : tile * 8 + 6, :] = field_ref[:, lanes]
        feat[tile * 8 + 6 : tile * 8 + 7, :] = polar_ref[:, lanes]
        feat[tile * 8 + 7 : tile * 8 + 8, :] = jnp.ones((1, width), F32)

    def fill(tile):
        value = gather_tile(atom_ref[pl.ds(tile, 1), :], feat, tiles)
        root = lax.rsqrt(value)
        window[eight(tile), :] = jnp.where(sub_ids == 7, pltpu.roll(root, 1, 0), value)

    grouped(8, fill)

    def copy_p():
        return pltpu.make_async_remote_copy(
            src_ref=sent_p,
            dst_ref=ahead_p,
            send_sem=pack_sem.at[0],
            recv_sem=pack_sem.at[1],
            device_id={"gx": before},
            device_id_type=MESH,
        )

    def copy_w(turn):
        return pltpu.make_async_remote_copy(
            src_ref=sent_w.at[turn],
            dst_ref=ahead_w.at[turn],
            send_sem=w_sem.at[0, turn],
            recv_sem=w_sem.at[1, turn],
            device_id={"gx": before},
            device_id_type=MESH,
        )

    pair_inputs = (0, 1, 2, 7)
    for at, row in enumerate(pair_inputs):
        sent_p[at] = window[strided(0, row), :]
    resid = [window[strided(0, 3 + axis), :] for axis in range(3)]
    for axis in range(3):
        sent_w[0, axis] = resid[axis]
    pl.semaphore_wait(barrier, count - 1)
    copy_p().start()
    copy_w(0).start()

    row_ids = lax.broadcasted_iota(jnp.int32, (width, width), 0)
    column_ids = lax.broadcasted_iota(jnp.int32, (width, width), 1)
    away[...] = jnp.where(row_ids == column_ids, AWAY, 0.0)

    def centre(first):
        whole = slice(first, first + tiles)
        ones = jnp.ones((tiles, width), F32)
        for axis in range(3):
            here = window[strided(first, axis), :]
            mean = jnp.floor(jnp.mean(here, axis=1, keepdims=True) + 0.5)
            mean = jnp.broadcast_to(mean, here.shape)
            middle[strided(first, axis), :] = mean
            here = here - mean
            local[axis, whole, :] = here
            bases[strided(first, axis), :] = here
            bases[strided(first, axis + 4), :] = here
        bases[strided(first, 3), :] = ones
        bases[strided(first, 7), :] = ones
        for row in range(3, 8):
            middle[strided(first, row), :] = jnp.zeros((tiles, width), F32)
        for tile in range(first, first + tiles):
            here = window[tile * 8 : tile * 8 + 8, :]
            root = jnp.broadcast_to(here[7:8, :], (8, width))
            placed[tile] = jnp.where(sub_ids < 3, here, jnp.where(sub_ids < 5, 0.0, root))
            centred[tile] = middle[tile * 8 : tile * 8 + 8, :]

    def split_rows(value):
        high = value.astype(BF16).astype(F32)
        rest = value - high
        middle = rest.astype(BF16).astype(F32)
        return high, middle, rest - middle

    def left_rows(tile):
        ones = jnp.ones((24, width), F32)
        return jnp.concatenate([*split_rows(placed[tile]), ones], axis=0).astype(BF16)

    def right_rows(other):
        high, mid, low = split_rows(jnp.where(sub_ids >= 5, other * -thole_factor, other))
        zero = jnp.zeros((8, width), F32)
        parts = []
        for axis in range(3):
            here = sub_ids == axis
            one = jnp.where(here, -1.0, 0.0)
            parts.append(
                [one, one, one] + [jnp.where(here, value, 0.0) for value in (high, mid, low)]
            )
        third = jnp.where(sub_ids == 7, high, 0.0)
        second = jnp.where(sub_ids == 6, mid, third)
        parts.append([jnp.where(sub_ids == 5, low, second), second, third, zero, zero, zero])
        parts = [jnp.concatenate(part, axis=0) for part in parts]
        return jnp.concatenate(parts, axis=1).astype(BF16)

    def offsets(left, right):
        return lax.dot_general(
            left, right, (((0,), (0,)), ((), ())), preferred_element_type=F32
        )

    def pair_rows(found, first, same):
        rows = slice(first, first + 16)
        off_x, off_y, off_z, scale = [
            found[rows, part * width : (part + 1) * width] for part in range(4)
        ]
        dist_sq = off_x * off_x + off_y * off_y + off_z * off_z
        if same:
            dist_sq = dist_sq + away[rows, :]
        inv = lax.rsqrt(dist_sq)
        inv_sq = inv * inv
        inv_cube = inv_sq * inv
        cube = dist_sq * (dist_sq * inv)
        decay = jnp.exp(scale * cube)
        three = inv_cube - inv_cube * decay
        five = inv_sq * (three + scale * decay)
        return three, five

    def store_pair(target, index, first, three, five):
        for at, value in ((first, five), (width + first, three)):
            for half, part in enumerate(split_two(value)):
                target[index, at : at + 16, half * width : (half + 1) * width] = part

    def put_coefs(index, shift):
        def row(at):
            return jnp.broadcast_to(-shift[at : at + 1, :], (8, width))

        coefs[index, 0] = jnp.where(low_rows, row(0), 1.0)
        coefs[index, 1] = jnp.where(low_rows, row(1), row(2))
        coefs[index, 2] = shift

    def own_pairs(tile):
        here = placed[tile]
        found = offsets(left_rows(tile), right_rows(here))
        for first in range(0, width, 16):
            three, five = pair_rows(found, first, True)
            store_pair(pair_own, tile, first, three, five)
        put_coefs(tile, here - centred[tile])

    centre(0)
    grouped(8, own_pairs)

    lane_ids = row_ids
    tile_ids = lax.broadcasted_iota(jnp.int32, (tiles, width), 0)
    lane_row = lax.broadcasted_iota(jnp.int32, (tiles, width), 1).astype(F32)
    found_ref[...] = jnp.zeros_like(found_ref)

    def invert(tile):
        row = atom_ref[pl.ds(tile, 1), :]
        outer = tile_ids == (row >> 7)
        number = jnp.full((tiles, width), tile, jnp.int32).astype(F32)
        left = jnp.concatenate(
            [jnp.where(outer, number, 0.0), jnp.where(outer, lane_row, 0.0)], axis=0
        ).astype(BF16)
        right = jnp.where(lane_ids == (row & (width - 1)), 1.0, 0.0).astype(BF16)
        return lax.dot_general(
            left, right, (((1,), (1,)), ((), ())), preferred_element_type=F32
        )

    def invert_step(group, carry):
        total = found_ref[...]
        for offset in range(8):
            total = total + invert(group * 8 + offset)
        found_ref[...] = total
        return carry

    lax.fori_loop(0, tiles // 8, invert_step, 0)
    inverse[...] = (found_ref[:tiles] * float(width) + found_ref[tiles:]).astype(jnp.int32)

    for arrival in arrivals[4:]:
        arrival.wait()
    copy_p().wait_recv()
    for at, row in enumerate(pair_inputs):
        window[strided(tiles, row), :] = ahead_p[at]
    centre(tiles)

    lengths = (jnp.where(me == count - 1, 4.0 * count, 0.0), 128.0, 2.0 * tiles)

    def far_pairs(tile):
        here = placed[tile]
        here_middle = centred[tile]
        left = left_rows(tile)
        for entry in range(near):
            slot = entry * tiles + tile
            named = list_ref[entry + 1, tile]
            crossing = jnp.full((8, width), named, jnp.int32) >= tiles
            moves = jnp.where(
                sub_ids == 0,
                jnp.where(crossing, lengths[0], 0.0),
                jnp.where(
                    sub_ids == 1,
                    shift_ref[entry + 1, 0, tile].astype(F32) * lengths[1],
                    jnp.where(sub_ids == 2, shift_ref[entry + 1, 1, tile].astype(F32) * lengths[2], 0.0),
                ),
            )
            other = placed[named] + moves
            put_coefs(tiles + slot, other - here_middle)
            put_coefs(tiles + slots + slot, here - (centred[named] + moves))
            found = offsets(left, right_rows(other))
            for first in range(0, width, 16):
                three, five = pair_rows(found, first, False)
                store_pair(pair_back, slot, first, three, five)
            for half in range(2):
                for part in (slice(0, width), slice(width, 2 * width)):
                    lanes = slice(half * width, (half + 1) * width)
                    pair_left[slot, part, lanes] = pair_back[slot, part, lanes].T


    named_row = jnp.concatenate(
        [names_ref[entry + 1 : entry + 2, :] for entry in range(near)] * 3, axis=1
    )
    window_ids = lax.broadcasted_iota(jnp.int32, (2 * tiles, 3 * slots), 0)
    hits = jnp.where(window_ids == named_row, 1.0, 0.0).astype(BF16)

    alpha_inv = 1.0 / window[strided(0, 6), :]

    def put_vector(first, vec):
        whole = slice(first, first + tiles)
        along = local[0, whole, :] * vec[0] + local[1, whole, :] * vec[1] + local[2, whole, :] * vec[2]
        for axis in range(3):
            vectors[strided(first, axis), :] = 3.0 * vec[axis]
            vectors[strided(first, axis + 4), :] = -vec[axis]
        vectors[strided(first, 3), :] = 3.0 * along

    vectors[...] = jnp.zeros_like(vectors)

    def make_block(tile):
        base = bases[eight(tile), :]
        vec = vectors[eight(tile), :]

        def row(at):
            return jnp.broadcast_to(vec[at : at + 1, :], (8, width))

        moments = jnp.concatenate(
            [
                base * jnp.where(low_rows, row(0), row(3)),
                base * jnp.where(low_rows, row(1), row(2)),
            ],
            axis=0,
        )
        minus = jnp.concatenate([jnp.where(low_rows, 0.0, vec), jnp.zeros((8, width), F32)], axis=0)
        for part, value in enumerate(split_three(moments)):
            blocks[tile, 0, part * 16 : part * 16 + 16, :] = value
        for part, value in enumerate(split_three(minus)):
            blocks[tile, 1, part * 16 : part * 16 + 16, :] = value

    def product(tile, pairs, slot, index):
        block = blocks[tile]
        weights = pairs[slot]
        out = jnp.dot(
            jnp.concatenate([block[0], block[1]], axis=1),
            weights,
            preferred_element_type=F32,
        )
        out = out[:, :width] + out[:, width:]
        out = (out[0:16] + out[16:32]) + out[32:48]
        total = coefs[index, 0] * out[0:8] + coefs[index, 1] * out[8:16]
        total = total + pltpu.roll(total, 4, 0)
        return total - coefs[index, 2] * jnp.broadcast_to(total[3:4, :], (8, width))

    def copy_f(turn):
        return pltpu.make_async_remote_copy(
            src_ref=sent_f.at[turn],
            dst_ref=back_f.at[turn],
            send_sem=f_sem.at[0, turn],
            recv_sem=f_sem.at[1, turn],
            device_id={"gx": after},
            device_id_type=MESH,
        )

    def back_step(tile):
        make_block(tile)
        for entry in range(near):
            slot = entry * tiles + tile
            fields[eight(slot), :] = product(tile, pair_back, slot, tiles + slot)

    def own_step(tile):
        summed[eight(tile), :] = product(tile, pair_own, tile, tile)

    def left_step(tile):
        total = summed[eight(tile), :]
        for entry in range(near):
            slot = entry * tiles + tile
            named = list_ref[entry + 1, tile]
            total = total + product(named, pair_left, slot, tiles + slots + slot)
        summed[eight(tile), :] = total

    put_vector(0, resid)

    def far_group(group, carry):
        for offset in range(FAR):
            back_step(lax.rem(group * FAR + offset + tiles - FAR, tiles))
        for offset in range(FAR):
            far_pairs(group * FAR + offset)
        return carry

    lax.fori_loop(0, tiles // FAR, far_group, 0)
    for offset in range(FAR):
        back_step(tiles - FAR + offset)

    def applied(turn, vec, meanwhile=None):
        if turn > 0:
            put_vector(0, vec)
            grouped(32, back_step)
        back = jnp.concatenate(
            [fields[pl.ds(axis, slots, stride=8), :] for axis in range(3)], axis=1
        )
        spread = jnp.dot(
            hits, jnp.concatenate(split_three(back), axis=0), preferred_element_type=F32
        )
        for axis in range(3):
            sent_f[turn, axis] = spread[tiles:, axis * width : (axis + 1) * width]
        copy_f(turn).start()
        if meanwhile is not None:
            meanwhile()
        grouped(32, own_step)
        copy_w(turn).wait_recv()
        ahead = [ahead_w[turn, axis] for axis in range(3)]
        put_vector(tiles, ahead)
        for tile in range(tiles):
            make_block(tiles + tile)
        grouped(32, left_step)
        field = [
            summed[strided(0, axis), :] + spread[:tiles, axis * width : (axis + 1) * width]
            for axis in range(3)
        ]
        return [vec[axis] * alpha_inv - field[axis] for axis in range(3)]

    first_half = lax.broadcasted_iota(jnp.int32, (1, width), 1) < width // 2

    def dot_rows(left, right):
        total = left[0] * right[0] + left[1] * right[1] + left[2] * right[2]
        return jnp.sum(total, axis=0, keepdims=True)

    def send_dots(turn, resid, w):
        norm_row, product_row = dot_rows(resid, resid), dot_rows(resid, w)
        dots[turn, 0] = jnp.where(
            first_half,
            norm_row + pltpu.roll(norm_row, width // 2, 1),
            product_row + pltpu.roll(product_row, width // 2, 1),
        )

        def send(step, carry):
            pltpu.make_async_remote_copy(
                src_ref=dots.at[turn, 0],
                dst_ref=dots.at[turn, step],
                send_sem=dot_sem.at[0, turn],
                recv_sem=dot_sem.at[1, turn],
                device_id={"gx": lax.rem(me + step, count)},
                device_id_type=MESH,
            ).start()
            return carry

        lax.fori_loop(1, count, send, 0)

    def wait_dots(turn, which):
        whole = dots.at[turn, pl.ds(1, count - 1)]
        pltpu.make_async_copy(whole, whole, dot_sem.at[which, turn]).wait()

    def gather_last(solution, resid, direction, w, s):
        for axis in range(3):
            feat[strided(0, axis), :] = solution[axis]
            feat[strided(0, 3 + axis), :] = resid[axis]
            feat[strided(tiles, axis), :] = direction[axis]
            feat[strided(tiles, 3 + axis), :] = s[axis]
        for row, part in ((6, w[0]), (7, w[1]), (8 * tiles + 6, w[2])):
            feat[pl.ds(row, tiles, stride=8), :] = part

        feat[strided(tiles, 7), :] = w[2]

        def fetch(tile):
            row = inverse[pl.ds(tile, 1), :]
            final[eight(tile), :] = gather_tile(row, feat, tiles)
            final[eight(tiles + tile), :] = gather_tile(row, feat, tiles, tiles)

        grouped(4, fetch)

    w = applied(0, resid)
    copy_f(0).wait_recv()
    w = [w[axis] - back_f[0, axis] for axis in range(3)]
    solution = direction = s = z = None
    norm_last = step_last = None
    for turn in range(ITERS):
        more_turns = turn + 1 < ITERS
        if more_turns:
            for axis in range(3):
                sent_w[turn + 1, axis] = w[axis]
            copy_w(turn + 1).start()
            send_dots(turn, resid, w)
            q = applied(turn + 1, w)
        else:
            send_dots(turn, resid, w)
            gather_last(solution, resid, direction, w, s)
        wait_dots(turn, 1)
        sums = jnp.sum(dots[turn], axis=0)
        norm = jnp.sum(jnp.where(first_half, sums, 0.0), axis=1, keepdims=True)
        product_now = jnp.sum(jnp.where(first_half, 0.0, sums), axis=1, keepdims=True)
        if turn == 0:
            step = norm / product_now
            direction, s = resid, w
            solution = [step * direction[axis] for axis in range(3)]
            if more_turns:
                z = q
        else:
            ratio = norm / norm_last
            step = norm / (product_now - ratio * norm / step_last)
            if not more_turns:
                break
            direction = [resid[axis] + ratio * direction[axis] for axis in range(3)]
            s = [w[axis] + ratio * s[axis] for axis in range(3)]
            solution = [solution[axis] + step * direction[axis] for axis in range(3)]
            z = [q[axis] + ratio * z[axis] for axis in range(3)]
        resid = [resid[axis] - step * s[axis] for axis in range(3)]
        if more_turns:
            w = [w[axis] - step * z[axis] for axis in range(3)]
            copy_f(turn + 1).wait_recv()
            late = [back_f[turn + 1, axis] for axis in range(3)]
            w = [w[axis] + step * late[axis] for axis in range(3)]
            z = [z[axis] - late[axis] for axis in range(3)]
        norm_last, step_last = norm, step

    plus = jnp.where(sub_ids < 3, 1.0, -1.0)
    by_ratio = plus * (step * ratio)
    by_step = plus * step

    def give(tile):
        first, second = final[eight(tile), :], final[eight(tiles + tile), :]
        third = jnp.where(sub_ids == 5, pltpu.roll(second, 7, 0), pltpu.roll(first, 5, 0))
        value = first + by_step * third + by_ratio * second
        lanes = pl.ds(pl.multiple_of(tile * width, width), width)
        out_ref[:, lanes] = value[0:6]

    grouped(8, give)

    copy_p().wait_send()
    for turn in range(ITERS):
        copy_w(turn).wait_send()
        copy_f(turn).wait_send()
        wait_dots(turn, 0)
    leave = pltpu.make_async_copy(out_ref, out_any, out_sem)
    leave.start()
    leave.wait()


def on_device(positions, polar, field_ext, tile_atom, tile_list, image_shift):
    tiles, links = tile_list.shape
    atoms = tile_atom.shape[0]
    width = atoms // tiles
    near = links - 1
    count = lax.axis_size("gx")
    pairs = (2 * width, 2 * width)
    out = jax.ShapeDtypeStruct((6, atoms), F32)
    vectors = pltpu.VMEM((ITERS, 3, tiles, width), F32)
    per_slab = pltpu.VMEM((tiles * 8, width), F32)
    per_window = pltpu.VMEM((2 * tiles * 8, width), F32)
    names = tile_list.T
    both = pl.pallas_call(
        functools.partial(kernel, count, tiles, links),
        out_shape=out,
        in_specs=[pl.BlockSpec(memory_space=pltpu.HBM)] * 6,
        out_specs=pl.BlockSpec(memory_space=pl.ANY),
        scratch_shapes=[
            pltpu.SMEM((links, tiles), jnp.int32),
            pltpu.SMEM((links, 2, tiles), jnp.int32),
            pltpu.VMEM((links, tiles), jnp.int32),
            pltpu.VMEM((3, atoms), F32),
            pltpu.VMEM((1, atoms), F32),
            pltpu.VMEM((3, atoms), F32),
            pltpu.VMEM((tiles, width), jnp.int32),
            pltpu.VMEM((6, atoms), F32),
            pltpu.SemaphoreType.DMA((7,)),
            pltpu.SemaphoreType.DMA,
            per_window,
            pltpu.VMEM((tiles, width), jnp.int32),
            per_window,
            pltpu.VMEM((2 * tiles, width), F32),
            per_window,
            per_window,
            pltpu.VMEM((2 * tiles, 8, width), F32),
            pltpu.VMEM((2 * tiles, 8, width), F32),
            pltpu.VMEM((3, 2 * tiles, width), F32),
            pltpu.VMEM((width, width), F32),
            pltpu.VMEM((tiles,) + pairs, BF16),
            pltpu.VMEM((near * tiles,) + pairs, BF16),
            pltpu.VMEM((near * tiles,) + pairs, BF16),
            per_window,
            pltpu.VMEM(((1 + 2 * near) * tiles, 3, 8, width), F32),
            per_window,
            pltpu.VMEM((2 * tiles, 2, 48, width), BF16),
            pltpu.VMEM((near * tiles * 8, width), F32),
            per_slab,
            pltpu.VMEM((4, tiles, width), F32),
            pltpu.VMEM((4, tiles, width), F32),
            vectors,
            vectors,
            vectors,
            vectors,
            pltpu.VMEM((ITERS, count, 1, width), F32),
            pltpu.SemaphoreType.DMA((2,)),
            pltpu.SemaphoreType.DMA((2, ITERS)),
            pltpu.SemaphoreType.DMA((2, ITERS)),
            pltpu.SemaphoreType.DMA((2, ITERS)),
        ],
        compiler_params=pltpu.CompilerParams(
            collective_id=0, has_side_effects=True
        ),
    )(
        names,
        image_shift.transpose(2, 0, 1),
        positions,
        polar.reshape(1, atoms),
        field_ext,
        tile_atom.reshape(tiles, width),
    )
    return both[:3], both[3:]


def solution(mesh):
    in_specs = (
        P(None, ("rep", "gx")),
        P(("rep", "gx")),
        P(None, ("rep", "gx")),
        P(("rep", "gx")),
        P(("rep", "gx"), None),
        P(None, ("rep", "gx"), None),
    )
    out_specs = (P(None, ("rep", "gx")), P(None, ("rep", "gx")))
    return jax.shard_map(
        on_device, mesh=mesh, in_specs=in_specs, out_specs=out_specs, check_vma=False
    )
```
